32 devices in a mesh: clump: 8 (over z, y), grp: 4 (over x, core).
Axes of the slice: x: 2, y: 2, z: 4, core: 2. Of those that a mesh axis runs over, the one named last changes fastest.
Arguments:
- flux: float32 [32, 1024, 64], P(('clump', 'grp')), may hold values from -6 to 6
- patch_pft: int32 [32, 1024], P(('clump', 'grp')), may hold values from 0 to 15
- patch_wt: float32 [32, 1024], P(('clump', 'grp')), may hold values from 0.2 to 2
- patch_col: int32 [32, 1024], P(('clump', 'grp')), may hold values from 0 to 511, never falling along the last dimension, each value on 1 to 4 neighbouring positions
- col_wt: float32 [32, 512], P(('clump', 'grp')), may hold values from 0.2 to 2
- col_lu: int32 [32, 512], P(('clump', 'grp')), may hold values from 0 to 255, never falling along the last dimension, each value on 1 to 4 neighbouring positions
- lu_wt: float32 [32, 256], P(('clump', 'grp')), may hold values from 0.2 to 2
- lu_grid: int32 [32, 256], P(('clump', 'grp')), may hold values from 0 to 127, never falling along the last dimension, each value on 1 to 4 neighbouring positions
- cell_target: int32 [32, 128], P(('clump', 'grp')), may hold values from 0 to 4095, as said below
- patch_count: int32 [32], P(('clump', 'grp')), may hold values from 64 to 1024
- pft_scale: float32 [16, 64], replicated, may hold values from 0.3 to 3
- cpl_frac: float32 [4096], P(('clump', 'grp')), may hold values from 0.2 to 0.9
- cpl_field: float32 [4096, 64], P(('clump', 'grp')), may hold values from -6 to 6
Outputs:
- grid_merged: float32 [4096, 64], P(('clump', 'grp'))
- anomaly: float32 [32, 1024, 64], P(('clump', 'grp'))
The draws below stay inside these ranges and needn't reach their ends.
Inputs may be any that keep to these rules, and one draw needn't show every extreme that they name: `patch_col`: within each device's row the column numbers never fall, and each column holds 1 to 4 patch slots. `col_lu`: within each device's row the landunit numbers never fall, and each landunit holds 1 to 4 columns. `lu_grid`: within each device's row the gridcell numbers never fall, and each gridcell holds 1 to 4 landunits. `cell_target`: all devices' entries together are a permutation of 0 to 4095; the coupler owner of an entry q is q // 128, and each device's 128 gridcells go to 16 owners, exactly 8 to each.
All inputs are finite; a program needn't handle non-finite values.
Results may differ from the reference program's by a relative error of at most 0.0003.
Values sent between devices are 32-bit elements; how exact they have to be, the bound alone decides.
A program may use at most 64 MiB of HBM per device.

```python
import math
import jax
import jax.numpy as jnp
import numpy as np
from jax import lax

NV = 64
NPFT = 16
P_DEV = 1024
C_DEV = 512
L_DEV = 256
G_DEV = 128
CAP = 8
GRID = 4096
DEVICES = 32


def row_orders(key, rows, length):

    def single(row_key):
        return jax.random.permutation(row_key, length)
    return jax.vmap(single)(jax.random.split(key, rows))


def draw_cell_target(key, part):
    key_shift, key_label, key_local, key_slot = jax.random.split(jax.random.fold_in(key, 11), 4)
    shift = jax.random.permutation(key_shift, DEVICES).astype(jnp.int32)
    label = jax.random.permutation(key_label, DEVICES).astype(jnp.int32)
    local_order = row_orders(key_local, DEVICES, G_DEV).astype(jnp.int32)
    slot_order = row_orders(key_slot, DEVICES, G_DEV).astype(jnp.int32)
    block_of = local_order // CAP
    pre_owner = (block_of + shift[:, None]) % DEVICES
    owner_dev = label[pre_owner]
    slot_in = slot_order[pre_owner, local_order]
    return (owner_dev * G_DEV + slot_in).astype(jnp.int32)


def place_ends(result, key, least, largest):
    index_at = [jax.random.randint(jax.random.fold_in(key, axis), (), 0, length) for axis, length in enumerate(result.shape)]
    widest = result.shape.index(max(result.shape))
    beside = index_at[:widest] + [(index_at[widest] + 1) % result.shape[widest]] + index_at[widest + 1:]
    return result.at[tuple(index_at)].set(least).at[tuple(beside)].set(largest)


def steps_of(key, dims, cuts, smallest, high):
    factor_of = 1.0
    for dim, parts in cuts:
        steps = jax.random.uniform(jax.random.fold_in(jax.random.fold_in(key, 6), dim), (parts,), jnp.float32, smallest / len(cuts), high / len(cuts))
        factor_of = factor_of * jnp.repeat(jnp.exp(steps), dims[dim] // parts).reshape((-1,) + (1,) * (len(dims) - 1 - dim))
    return factor_of


def split_up(count, total, most, lean):
    loads = [(1 << 20) // math.isqrt(standing ** lean) + 1 for standing in range(2, count + 1)]
    spare, counts = total - most - (count - 1), [1] * (count - 1)
    while spare > 0:
        candidates = [i for i in range(count - 1) if counts[i] < most]
        mass, left = sum([loads[i] for i in candidates]), spare
        for i in candidates:
            more = min(most - counts[i], max(1, left * loads[i] // mass), spare)
            counts[i] = counts[i] + more
            spare = spare - more
    return np.array([most] + counts)


def ragged(own_key, number_of, total, most, slope):
    if number_of == 2:
        one = jax.random.randint(own_key, (), max(1, total - most), min(most, total - 1) + 1)
        return jnp.stack([one, total - one])
    tallies = jnp.asarray(split_up(number_of, total, most, slope), jnp.int32)
    couples = (number_of - 1) // 2
    giver, sink = tallies[1:1 + 2 * couples:2], tallies[2:2 + 2 * couples:2]
    margin = jnp.minimum(giver - 1, most - sink)
    passed = jax.random.randint(jax.random.fold_in(own_key, 1), (couples,), 0, 1 << 20) % (margin + 1)
    tallies = tallies.at[1:1 + 2 * couples:2].set(giver - passed).at[2:2 + 2 * couples:2].set(sink + passed)
    return tallies[jax.random.permutation(jax.random.fold_in(own_key, 2), number_of)]


def gaussian(rng, dims, deviation, reach, pieces=(), kind=jnp.bfloat16):
    factor_of = steps_of(rng, dims, pieces, -0.22, 0.18) if pieces else 1.0
    array = jax.random.normal(rng, dims, jnp.float32) * deviation * factor_of
    return jnp.minimum(jnp.maximum(array, -reach), reach).astype(kind)


def setup_inputs(seed: int = 0) -> dict:
    seeds = jax.random.split(jax.random.key(seed), 14)
    flux = gaussian(seeds[0], (DEVICES, P_DEV, NV), 1.0, 6.0, ((0, 32),), jnp.float32)
    patch_pft = place_ends(jax.random.randint(seeds[1], (DEVICES, P_DEV), 0, NPFT), jax.random.fold_in(seeds[1], 1), 0, NPFT - 1).astype(jnp.int32)
    patch_wt = jnp.clip(jnp.exp(math.log(2.0) - 2.3025851 * jax.random.uniform(seeds[2], (DEVICES, P_DEV), jnp.float32) ** steps_of(seeds[2], (DEVICES, P_DEV), ((0, 32),), -0.2, 0.2)), 0.2, 2.0)
    patch_col = jax.vmap(lambda own: jnp.searchsorted(jnp.cumsum(ragged(own, C_DEV, P_DEV, 4, 1)), jnp.arange(P_DEV), side="right"))(jax.random.split(seeds[3], DEVICES)).reshape((DEVICES, P_DEV)).astype(jnp.int32)
    col_wt = jnp.clip(jnp.exp(math.log(2.0) - 2.3025851 * jax.random.uniform(seeds[4], (DEVICES, C_DEV), jnp.float32) ** steps_of(seeds[4], (DEVICES, C_DEV), ((0, 32),), -0.2, 0.2)), 0.2, 2.0)
    col_lu = jax.vmap(lambda own: jnp.searchsorted(jnp.cumsum(ragged(own, L_DEV, C_DEV, 4, 1)), jnp.arange(C_DEV), side="right"))(jax.random.split(seeds[5], DEVICES)).reshape((DEVICES, C_DEV)).astype(jnp.int32)
    lu_wt = jnp.clip(jnp.exp(math.log(2.0) - 2.3025851 * jax.random.uniform(seeds[6], (DEVICES, L_DEV), jnp.float32) ** steps_of(seeds[6], (DEVICES, L_DEV), ((0, 32),), -0.2, 0.2)), 0.2, 2.0)
    lu_grid = jax.vmap(lambda own: jnp.searchsorted(jnp.cumsum(ragged(own, G_DEV, L_DEV, 4, 1)), jnp.arange(L_DEV), side="right"))(jax.random.split(seeds[7], DEVICES)).reshape((DEVICES, L_DEV)).astype(jnp.int32)
    cell_target = draw_cell_target(jax.random.fold_in(seeds[13], 71), 0)
    patch_count = place_ends(jax.random.randint(seeds[9], (DEVICES,), P_DEV // 16, P_DEV + 1), jax.random.fold_in(seeds[9], 1), P_DEV // 16, P_DEV).astype(jnp.int32)
    pft_scale = jnp.clip(jnp.exp(jax.random.uniform(seeds[10], (NPFT, NV), jnp.float32, math.log(0.3), math.log(3.0))), 0.3, 3.0)
    cpl_frac = jnp.clip(0.2 + 0.7 * jax.random.uniform(seeds[11], (GRID,), jnp.float32) ** steps_of(seeds[11], (GRID,), ((0, 32),), -0.2, 0.2), 0.2, 0.9)
    cpl_field = gaussian(seeds[12], (GRID, NV), 1.0, 6.0, ((0, 32),), jnp.float32)
    return {"flux": flux, "patch_pft": patch_pft, "patch_wt": patch_wt, "patch_col": patch_col, "col_wt": col_wt, "col_lu": col_lu, "lu_wt": lu_wt, "lu_grid": lu_grid, "cell_target": cell_target, "patch_count": patch_count, "pft_scale": pft_scale, "cpl_frac": cpl_frac, "cpl_field": cpl_field}


def reference(flux, patch_pft, patch_wt, patch_col, col_wt, col_lu, lu_wt, lu_grid, cell_target, patch_count, pft_scale, cpl_frac, cpl_field):
    position = jnp.arange(P_DEV, dtype=jnp.int32)

    def local_means(entries):
        values, pft_ids, pweight, columns, cweight, colland, lweight, lugrid, live_count = entries
        alive_mask = (position < live_count).astype(jnp.float32)
        scaled = values * pft_scale[pft_ids]
        land_of = colland[columns]
        home_of = lugrid[land_of]
        weight_eff = alive_mask * pweight * cweight[columns] * lweight[land_of]
        numer = jax.ops.segment_sum(scaled * weight_eff[:, None], home_of, G_DEV)
        denom = jax.ops.segment_sum(weight_eff, home_of, G_DEV)
        return numer / jnp.maximum(denom, 1.0)[:, None]

    cell_mean = lax.map(local_means, (flux, patch_pft, patch_wt, patch_col, col_wt, col_lu, lu_wt, lu_grid, patch_count))
    placed = jnp.zeros((GRID, NV), jnp.float32).at[cell_target.reshape(-1)].set(cell_mean.reshape(-1, NV))
    grid_merged = cpl_frac[:, None] * placed + (1.0 - cpl_frac)[:, None] * cpl_field

    def local_anomaly(entries):
        values, pft_ids, columns, colland, lugrid, targets, live_count = entries
        alive_mask = (position < live_count).astype(jnp.float32)
        scaled = values * pft_scale[pft_ids]
        home_of = lugrid[colland[columns]]
        cell_merged = grid_merged[targets]
        return alive_mask[:, None] * (scaled - cell_merged[home_of])

    anomaly = lax.map(local_anomaly, (flux, patch_pft, patch_col, col_lu, lu_grid, cell_target, patch_count))
    return grid_merged, anomaly
```

```python
import functools

import jax
import jax.numpy as jnp
from jax import lax
from jax.experimental import pallas as pl
from jax.experimental.pallas import tpu as pltpu
from jax.sharding import PartitionSpec as P

MESH = pl.DeviceIdType.MESH
F32 = jnp.float32
BF16 = jnp.bfloat16
INPUTS = 12


def iota(shape, dim):
    return lax.broadcasted_iota(jnp.int32, shape, dim)


def onehot(mask):
    return jnp.where(mask, 1.0, 0.0).astype(BF16)


def halves(x):
    high = x.astype(BF16)
    return high, (x - high.astype(F32)).astype(BF16)


def dot(a, b):
    return jnp.dot(a, b, preferred_element_type=F32)


def dot_nt(a, b):
    return lax.dot_general(a, b, (((1,), (1,)), ((), ())), preferred_element_type=F32)


def rows_of(rows, total):
    n = rows[0].shape[1]
    at = iota((total, n), 0)
    out = jnp.zeros((total, n), F32)
    for k, row in enumerate(rows):
        out = jnp.where(at == k, jnp.broadcast_to(row.astype(F32), (total, n)), out)
    return out.astype(BF16)


def split_by(x, size):
    if size & (size - 1) == 0:
        return lax.shift_right_logical(x, jnp.int32(size.bit_length() - 1)), x & (size - 1)
    return x // size, x % size


def select(table, chosen):
    high, low = halves(table)
    both = dot(jnp.concatenate([high, low], axis=0), chosen)
    return both[: table.shape[0]] + both[table.shape[0] :]


def pack_two(chosen, one, two):
    rows = chosen.shape[0] // 2
    pair = jnp.concatenate([chosen[:rows], chosen[rows:]], axis=1)
    blank = jnp.zeros(one.shape, BF16)

    def wide(first, second):
        upper = jnp.concatenate([first, blank], axis=1)
        return jnp.concatenate([upper, jnp.concatenate([blank, second], axis=1)], axis=0)

    (high, low), (high_two, low_two) = halves(one), halves(two)
    return dot_nt(pair, wide(high, high_two)) + dot_nt(pair, wide(low, low_two))


def pack(chosen, x):
    return pack_two(chosen, x, x)


def unpack(packed):
    turned = packed.T
    middle = turned.shape[0] // 2
    return jnp.concatenate([turned[:middle], turned[middle:]], axis=1)


def kernel(
    n_clump, n_group, inner_clump, inner_group, cap, slots, half, stride,
    *refs,
):
    count_ref, *refs = refs
    sources, refs = refs[:INPUTS], refs[INPUTS:]
    merged_ref, anomaly_ref = refs[:2]
    tables, ask, asked, reply, back, send, recv = refs[2:9]
    send_sem, recv_sem, in_sem, ready = refs[9:13]
    staged = refs[13:]
    (
        target_ref, lwt_ref, lgrid_ref, clu_ref, cwt_ref, pcol_ref, pwt_ref,
        scale_ref, pft_ref, flux_ref,
    ) = staged
    nv, patches = flux_ref.shape
    types = scale_ref.shape[0]
    cols = cwt_ref.shape[1]
    lus = lwt_ref.shape[1]
    cells = target_ref.shape[1]
    n = n_clump * n_group
    rows = n * stride
    outer_clump, outer_group = n_clump // inner_clump, n_group // inner_group
    sharers, askers = inner_clump * outer_group, outer_clump * inner_group
    pairs = sharers // 2
    field_ref, frac_ref = tables.at[0, pl.ds(0, nv)], tables.at[0, pl.ds(nv, 1)]
    loads = [
        pltpu.make_async_copy(source, into, in_sem.at[k])
        for k, (source, into) in enumerate(zip(sources, (*staged, frac_ref, field_ref)))
    ]
    my_clump, my_group = lax.axis_index("clump"), lax.axis_index("grp")
    my_slab, my_row = lax.div(my_clump, inner_clump), lax.rem(my_clump, inner_clump)
    my_side, my_core = lax.div(my_group, inner_group), lax.rem(my_group, inner_group)

    def ahead_of(mine, step, size):
        there = mine + step
        return jnp.where(there >= size, there - size, there)

    def behind(mine, step, size):
        there = mine - step
        return jnp.where(there < 0, there + size, there)

    def others(act, outer, inner):
        for i in range(1, inner):
            act(i, 0, i)
        if outer <= 8:
            for o in range(1, outer):
                for i in range(inner):
                    act(o * inner + i, o, i)
        else:

            @pl.loop(1, outer)
            def _(o):
                for i in range(inner):
                    act(o * inner + i, o, i)

    def each_sharer(act, there):
        def one(block, o, i):
            row, side = there(my_row, o, inner_clump), there(my_side, i, outer_group)
            act(block, (my_slab * inner_clump + row, side * inner_group + my_core))

        others(one, inner_clump, outer_group)

    def each_asker(act, there):
        def one(block, o, i):
            slab, core = there(my_slab, o, outer_clump), there(my_core, i, inner_group)
            act(block, (slab * inner_clump + my_row, my_side * inner_group + core))

        others(one, outer_clump, inner_group)

    def each_other(act, there):
        def one(block, o, i):
            act(block, (there(my_clump, o, n_clump), there(my_group, i, n_group)))

        others(one, n_clump, n_group)

    def remote(source, into, k, device):
        pltpu.make_async_remote_copy(
            src_ref=source,
            dst_ref=into,
            send_sem=send_sem.at[k],
            recv_sem=recv_sem.at[k],
            device_id=device,
            device_id_type=MESH,
        ).start()

    def wait(rest, sem):
        pltpu.make_async_copy(rest, rest, sem).wait()

    barrier = pltpu.get_barrier_semaphore()

    def greet(block, device):
        pl.semaphore_signal(barrier, inc=1, device_id=device, device_id_type=MESH)

    each_asker(greet, ahead_of)
    each_sharer(greet, ahead_of)
    for k in (11, 10, *range(10)):
        loads[k].start()

    table_rows = pl.ds(0, nv + 1)
    loads[10].wait()
    loads[11].wait()
    pl.semaphore_wait(barrier, sharers + askers - 2)

    def share(block, device):
        remote(tables.at[0, table_rows], tables.at[block, table_rows], 0, device)

    each_sharer(share, ahead_of)

    def tell(block, device):
        pl.semaphore_signal(ready, inc=1, device_id=device, device_id_type=MESH)

    each_sharer(tell, ahead_of)

    loads[0].wait()
    target = target_ref[...]
    owner, local = split_by(target, cells)
    owner_b = jnp.broadcast_to(owner.astype(F32), (cells, cells))
    same = owner_b == owner_b.T
    earlier = iota((cells, cells), 0) < iota((cells, cells), 1)
    rank = jnp.sum(jnp.where(same & earlier, 1.0, 0.0), axis=0, keepdims=True).astype(jnp.int32)
    to_clump, to_group = split_by(owner, n_group)
    to_slab, to_row = split_by(to_clump, inner_clump)
    to_side, to_core = split_by(to_group, inner_group)
    table = behind(my_row, to_row, inner_clump) * outer_group
    table = table + behind(my_side, to_side, outer_group)
    holder = behind(to_slab, my_slab, outer_clump) * inner_group
    holder = holder + behind(to_core, my_core, inner_group)
    wanted = (local + 1).astype(F32)
    asks = jnp.where(iota((askers, cells), 0) == holder, wanted, 0.0).astype(BF16)
    ask_rows = dot_nt(asks, onehot(iota((128, cells), 0) == table * slots + rank))
    for k in range(askers):
        ask[k, 0:1, :] = ask_rows[k : k + 1]
    asked[0, 0:1, :] = ask_rows[0:1]
    one_row = pl.ds(0, 1)

    def request(block, device):
        remote(ask.at[block, one_row], asked.at[block, one_row], 1, device)

    each_asker(request, ahead_of)

    frac = frac_ref[...]
    block = behind(to_clump, my_clump, n_clump) * n_group
    block = (block + behind(to_group, my_group, n_group)) * stride
    from_block = behind(my_clump, to_clump, n_clump) * n_group
    from_block = (from_block + behind(my_group, to_group, n_group)) * stride
    part, line = split_by(rank, half)
    slot_of = onehot(iota((2 * rows, cells), 0) == part * rows + block + line)
    at = iota((rows, cells), 0)
    asks = jnp.where(at == block + half, wanted, 0.0).astype(BF16)
    id_rows = dot_nt(asks, onehot(iota((128, cells), 0) == rank))
    in_stride = split_by(iota((rows, 128), 0), stride)[1]
    extra = jnp.where(in_stride == half + 1, jnp.broadcast_to(frac, (rows, cells)), id_rows)

    for load in loads[1:5]:
        load.wait()
    lu_hi, lu_lo = halves(lwt_ref[...])
    lu_rows = rows_of([lu_hi, lu_lo, lgrid_ref[...]], 16)
    lu_of = onehot(iota((lus, cols), 0) == clu_ref[...])
    col_vals = dot(lu_rows, lu_of)
    col_w = cwt_ref[...] * (col_vals[0:1] + col_vals[1:2])

    for load in loads[5:7]:
        load.wait()
    c_hi, c_lo = halves(col_w)
    col_rows = rows_of([c_hi, c_lo, col_vals[2:3]], 16)
    col_of = onehot(iota((cols, patches), 0) == pcol_ref[...])
    patch_vals = dot(col_rows, col_of)
    alive = jnp.where(iota((1, patches), 1) < count_ref[0], 1.0, 0.0)
    weight = alive * pwt_ref[...] * (patch_vals[0:1] + patch_vals[1:2])
    home = patch_vals[2:3].astype(jnp.int32)
    home_of = onehot(iota((cells, patches), 0) == home)

    for load in loads[7:10]:
        load.wait()
    scales = scale_ref[...]
    t1 = scales.astype(BF16).astype(F32)
    t2 = (scales - t1).astype(BF16).astype(F32)
    t3 = scales - t1 - t2
    pad = 128 - 3 * types
    stacked = jnp.concatenate([t1, t2, t3, jnp.zeros((pad, nv), F32)], axis=0)
    stacked = jnp.concatenate([stacked, jnp.zeros((128, 128 - nv), F32)], axis=1)
    scale_t = stacked.T[:nv].astype(BF16)
    kind = iota((128, patches), 0)
    type_of = onehot(
        (kind == pft_ref[...])
        | (kind == pft_ref[...] + types)
        | (kind == pft_ref[...] + 2 * types)
    )
    scaled = flux_ref[...] * dot(scale_t, type_of)

    x_hi, x_lo = halves(scaled * weight)
    w_hi, w_lo = halves(weight)
    sums = dot_nt(
        jnp.concatenate([x_hi, x_lo, rows_of([w_hi, w_lo], 16)], axis=0), home_of
    )
    num = sums[:nv] + sums[nv : 2 * nv]
    den = sums[2 * nv : 2 * nv + 1] + sums[2 * nv + 1 : 2 * nv + 2]
    mean = num / jnp.maximum(den, 1.0)

    send[...] = jnp.where(in_stride < half, pack(slot_of, mean), extra)
    lines = half + 2
    recv[0:lines, :] = send[0:lines, :]
    pl.semaphore_wait(ready, sharers - 1)

    def give(block, device):
        start = block * stride
        start = start if isinstance(start, int) else pl.multiple_of(start, stride)
        its = pl.ds(start, lines)
        remote(send.at[its], recv.at[its], 2, device)

    each_other(give, ahead_of)

    wait(asked.at[pl.ds(1, askers - 1), one_row], recv_sem.at[1])
    told = jnp.broadcast_to(asked[...][:, 0:1, :], (askers, slots, 128)).reshape(askers * slots, 128)
    lane_less = iota((askers * slots, 128), 1) - split_by(iota((askers * slots, 128), 0), slots)[1]
    spread = [jnp.where(lane_less == t * slots, told, 0.0) for t in range(sharers)]
    ids = dot(jnp.concatenate(spread, axis=0).astype(BF16), jnp.ones((128, cells), BF16))
    held_of = onehot(ids == (iota(ids.shape, 1) + 1).astype(F32))

    wait(tables.at[pl.ds(1, sharers - 1), table_rows], recv_sem.at[0])
    for p in range(pairs):
        one, two = 2 * p * askers * slots, (2 * p + 1) * askers * slots
        chosen = held_of[one : two + askers * slots]
        both = [(1.0 - tables[t, nv : nv + 1]) * tables[t, 0:nv] for t in (2 * p, 2 * p + 1)]
        reply[:, p * slots : (p + 1) * slots, :] = pack_two(chosen, *both).reshape(askers, slots, 128)
    back[0] = reply[0]

    def respond(block, device):
        remote(reply.at[block], back.at[block], 3, device)

    each_asker(respond, behind)

    other = (1.0 - frac) * field_ref[...]
    lane = iota((2 * rows, 128), 0)
    lane_part = jnp.where(lane >= rows, 1, 0)
    lane_line = split_by(lane - lane_part * rows, stride)[1]
    its_lane = (lane_line < half) & (
        iota((2 * rows, 128), 1) == lane_part * half + lane_line
    )
    pair, side = split_by(table, 2)
    place = side * (askers * pairs * slots) + (holder * pairs + pair) * slots + rank
    answer_of = onehot(iota((2 * askers * pairs * slots, cells), 0) == place)

    flat = [pl.ds(0, (n - 1) * lines), pl.ds(0, n * stride)]
    wait(recv.at[flat[0]], recv_sem.at[2])
    got = jnp.where(in_stride < lines, recv[...], 0.0)
    by_device = got.reshape(n, stride, 128)
    ids_of = jnp.broadcast_to(by_device[:, half : half + 1, :], (n, stride, 128)).reshape(rows, 128)
    spread = jnp.where(its_lane, jnp.concatenate([ids_of, ids_of], axis=0), 0.0).astype(BF16)
    ids = dot(spread, jnp.ones((128, cells), BF16))
    owned_of = onehot(ids == (iota((2 * rows, cells), 1) + 1).astype(F32))
    owned = select(unpack(jnp.where(in_stride < half, got, 0.0)), owned_of)
    merged_ref[...] = frac * owned + other

    all_frac = select(got.T, onehot(at == from_block + half + 1))
    cell_frac = jnp.sum(
        jnp.where(iota((128, cells), 0) == local, all_frac, 0.0), axis=0, keepdims=True
    )
    land_part = cell_frac * mean

    wait(back.at[pl.ds(1, askers - 1)], recv_sem.at[3])
    answers = back[...].reshape(askers * pairs * slots, 128)
    cell = land_part + select(unpack(answers), answer_of)
    anomaly_ref[...] = alive * (scaled - select(cell, home_of))
    wait(tables.at[pl.ds(1, sharers - 1), table_rows], send_sem.at[0])
    wait(ask.at[pl.ds(1, askers - 1), one_row], send_sem.at[1])
    wait(send.at[flat[0]], send_sem.at[2])
    wait(reply.at[pl.ds(1, askers - 1)], send_sem.at[3])


def store_kernel(merged, anomaly, merged_out, anomaly_out, sem):
    stores = [
        pltpu.make_async_copy(merged, merged_out, sem.at[0]),
        pltpu.make_async_copy(anomaly, anomaly_out, sem.at[1]),
    ]
    for store in stores:
        store.start()
    for store in stores:
        store.wait()


def per_device(
    flux, patch_pft, patch_wt, patch_col, col_wt, col_lu, lu_wt, lu_grid, cell_target,
    patch_count, pft_scale, cpl_frac, cpl_field,
):
    n_clump = lax.axis_size("clump")
    n_group = lax.axis_size("grp")
    n = n_clump * n_group
    nv = flux.shape[2]
    patches = flux.shape[1]
    cells = cell_target.shape[1]
    inner_group = 2 if n_group % 2 == 0 else 1
    outer_group = n_group // inner_group
    inner_clump = outer_group if n_clump % outer_group == 0 else 1
    sharers = inner_clump * outer_group
    askers = n // sharers
    cap = max(2, 2 * cells // n)
    half = -(-cap // 2)
    slots = -(-cap // 8) * 8
    stride = -(-(half + 2) // 8) * 8
    vmem = pl.BlockSpec(memory_space=pltpu.VMEM)
    hbm = pl.BlockSpec(memory_space=pltpu.HBM)
    staged = (
        cell_target, lu_wt, lu_grid, col_lu, col_wt, patch_col, patch_wt,
        pft_scale, patch_pft, flux[0].T,
    )
    inputs = (*staged, cpl_frac.reshape(1, -1), cpl_field.T)
    shapes = (
        jax.ShapeDtypeStruct((nv, cells), F32),
        jax.ShapeDtypeStruct((nv, patches), F32),
    )
    results = pl.pallas_call(
        functools.partial(
            kernel, n_clump, n_group, inner_clump, inner_group, cap, slots, half, stride
        ),
        out_shape=tuple(pltpu.VMEM(x.shape, x.dtype) for x in shapes),
        in_specs=[pl.BlockSpec(memory_space=pltpu.SMEM)] + [hbm] * INPUTS,
        out_specs=(vmem, vmem),
        scratch_shapes=[
            pltpu.VMEM((sharers, -(-(nv + 1) // 8) * 8, cells), F32),
            pltpu.VMEM((askers, 8, 128), F32),
            pltpu.VMEM((askers, 8, 128), F32),
            pltpu.VMEM((askers, sharers // 2 * slots, 128), F32),
            pltpu.VMEM((askers, sharers // 2 * slots, 128), F32),
            pltpu.VMEM((n * stride, 128), F32),
            pltpu.VMEM((n * stride, 128), F32),
            pltpu.SemaphoreType.DMA((4,)),
            pltpu.SemaphoreType.DMA((4,)),
            pltpu.SemaphoreType.DMA((INPUTS,)),
            pltpu.SemaphoreType.REGULAR,
        ]
        + [pltpu.VMEM(x.shape, x.dtype) for x in staged],
        compiler_params=pltpu.CompilerParams(
            collective_id=0, has_side_effects=True, vmem_limit_bytes=48 * 1024 * 1024
        ),
    )(patch_count, *[pltpu.with_memory_space_constraint(x, pltpu.HBM) for x in inputs])
    merged, anomaly = pl.pallas_call(
        store_kernel,
        out_shape=shapes,
        in_specs=[vmem, vmem],
        out_specs=(hbm, hbm),
        scratch_shapes=[pltpu.SemaphoreType.DMA((2,))],
        compiler_params=pltpu.CompilerParams(vmem_limit_bytes=4 * 1024 * 1024),
    )(*results)
    return merged.T, anomaly.T[None]


def solution(mesh):
    split = P(("clump", "grp"))
    return jax.shard_map(
        per_device,
        mesh=mesh,
        in_specs=(split,) * 10 + (P(),) + (split,) * 2,
        out_specs=(split, split),
        check_vma=False,
    )
```

```python
import functools

import jax
import jax.numpy as jnp
from jax import lax
from jax.experimental import pallas as pl
from jax.experimental.pallas import tpu as pltpu
from jax.sharding import PartitionSpec as P

MESH = pl.DeviceIdType.MESH
F32 = jnp.float32
BF16 = jnp.bfloat16
INPUTS = 12


def iota(shape, dim):
    return lax.broadcasted_iota(jnp.int32, shape, dim)


def onehot(mask):
    return jnp.where(mask, 1.0, 0.0).astype(BF16)


def halves(x):
    high = x.astype(BF16)
    return high, (x - high.astype(F32)).astype(BF16)


def dot(a, b):
    return jnp.dot(a, b, preferred_element_type=F32)


def dot_nt(a, b):
    return lax.dot_general(a, b, (((1,), (1,)), ((), ())), preferred_element_type=F32)


def rows_of(rows, total):
    n = rows[0].shape[1]
    at = iota((total, n), 0)
    out = jnp.zeros((total, n), F32)
    for k, row in enumerate(rows):
        out = jnp.where(at == k, jnp.broadcast_to(row.astype(F32), (total, n)), out)
    return out.astype(BF16)


def split_by(x, size):
    if size & (size - 1) == 0:
        return lax.shift_right_logical(x, jnp.int32(size.bit_length() - 1)), x & (size - 1)
    return x // size, x % size


def select(table, chosen):
    high, low = halves(table)
    both = dot(jnp.concatenate([high, low], axis=0), chosen)
    return both[: table.shape[0]] + both[table.shape[0] :]


def wide(one, two):
    blank = jnp.zeros(one.shape, BF16)

    def beside(first, second):
        upper = jnp.concatenate([first, blank], axis=1)
        return jnp.concatenate([upper, jnp.concatenate([blank, second], axis=1)], axis=0)

    (high, low), (high_two, low_two) = halves(one), halves(two)
    return beside(high, high_two), beside(low, low_two)


def pack_wide(chosen, parts):
    rows = chosen.shape[0] // 2
    pair = jnp.concatenate([chosen[:rows], chosen[rows:]], axis=1)
    return dot_nt(pair, parts[0]) + dot_nt(pair, parts[1])


def pack(chosen, x):
    return pack_wide(chosen, wide(x, x))


def unpack(packed):
    turned = packed.T
    middle = turned.shape[0] // 2
    return jnp.concatenate([turned[:middle], turned[middle:]], axis=1)


def kernel(
    n_clump, n_group, inner_clump, inner_group, cap, slots, half, stride,
    *refs,
):
    count_ref, *refs = refs
    sources, refs = refs[:INPUTS], refs[INPUTS:]
    merged_ref, anomaly_ref = refs[:2]
    tables, own, ask, asked, note, noted, reply, back, send, recv = refs[2:12]
    send_sem, recv_sem, in_sem, known, column = refs[12:17]
    staged = refs[17:]
    (
        target_ref, lwt_ref, lgrid_ref, clu_ref, cwt_ref, pcol_ref, pwt_ref,
        scale_ref, pft_ref, flux_ref,
    ) = staged
    nv, patches = flux_ref.shape
    types = scale_ref.shape[0]
    cols = cwt_ref.shape[1]
    lus = lwt_ref.shape[1]
    cells = target_ref.shape[1]
    n = n_clump * n_group
    rows = n * stride
    outer_clump, outer_group = n_clump // inner_clump, n_group // inner_group
    places, askers = inner_clump * outer_group, outer_clump * inner_group
    sharers = places * inner_group
    pairs = sharers // 2
    field_ref, frac_ref = own.at[pl.ds(0, nv)], own.at[pl.ds(nv, 1)]
    loads = [
        pltpu.make_async_copy(source, into, in_sem.at[k])
        for k, (source, into) in enumerate(zip(sources, (*staged, frac_ref, field_ref)))
    ]
    my_clump, my_group = lax.axis_index("clump"), lax.axis_index("grp")
    my_slab, my_row = lax.div(my_clump, inner_clump), lax.rem(my_clump, inner_clump)
    my_side, my_core = lax.div(my_group, inner_group), lax.rem(my_group, inner_group)
    keeper = inner_group - 1
    keeps = my_core == keeper

    def ahead_of(mine, step, size):
        there = mine + step
        return jnp.where(there >= size, there - size, there)

    def behind(mine, step, size):
        there = mine - step
        return jnp.where(there < 0, there + size, there)

    def offsets(act, outer, inner, own=False, far_first=False):
        if outer <= 8:
            steps = [(o, i) for o in range(outer) for i in range(inner) if own or o or i]
            for o, i in steps[::-1] if far_first else steps:
                act(o * inner + i, o, i)
        else:
            for i in range(0 if own else 1, inner):
                act(i, 0, i)

            @pl.loop(1, outer)
            def _(o):
                for i in range(inner):
                    act(o * inner + i, o, i)

    def place(there, row, side, slab, core):
        slab, row = there(my_slab, slab, outer_clump), there(my_row, row, inner_clump)
        side, core = there(my_side, side, outer_group), there(my_core, core, inner_group)
        return slab * inner_clump + row, side * inner_group + core

    def each_other(act, there):
        for row in range(inner_clump - 1, -1, -1):
            for side in range(outer_group - 1, -1, -1):
                t = row * outer_group + side

                def one(block, o, i, t=t, row=row, side=side):
                    act(t * askers + block, place(there, row, side, o, i))

                offsets(one, outer_clump, inner_group, own=t > 0)

    def remote(source, into, k, device):
        pltpu.make_async_remote_copy(
            src_ref=source,
            dst_ref=into,
            send_sem=send_sem.at[k],
            recv_sem=recv_sem.at[k],
            device_id=device,
            device_id_type=MESH,
        ).start()

    def wait(rest, sem):
        pltpu.make_async_copy(rest, rest, sem).wait()

    barrier = pltpu.get_barrier_semaphore()

    def signal(sem, device):
        pl.semaphore_signal(sem, inc=1, device_id=device, device_id_type=MESH)

    def when_places(act, there, first, second):
        def one(block, o, i):
            @pl.when((first + o < inner_clump) & (second + i < outer_group))
            def _():
                act(block, place(there, o, i, 0, 0))

        offsets(one, inner_clump, outer_group)

    def slabs(act):
        if outer_clump <= 8:
            for o in range(1, outer_clump):
                act(o)
        else:
            pl.loop(1, outer_clump)(act)

    def when_slabs(act, there, first):
        def one(o):
            @pl.when(first + o < outer_clump)
            def _():
                act(o, place(there, 0, 0, o, 0))

        slabs(one)

    def keeper_of(device):
        return device[0], device[1] - my_core + keeper

    def greet(block, device):
        signal(barrier, keeper_of(device))

        @pl.when(keeps)
        def _():
            for core in range(keeper):
                signal(barrier, (device[0], device[1] - my_core + core))

    up_row, up_side = inner_clump - 1 - my_row, outer_group - 1 - my_side
    up_slab = outer_clump - 1 - my_slab
    last_place, last_plane = up_row + up_side == 0, up_slab == 0
    last = last_place & last_plane & keeps
    when_slabs(greet, ahead_of, my_slab)
    when_places(greet, ahead_of, my_row, my_side)
    mates = [(my_clump, my_group - my_core + core) for core in range(inner_group)]

    @pl.when(keeps)
    def _():
        for core in range(keeper):
            signal(barrier, mates[core])

    @pl.when((last_place == last_plane) & jnp.logical_not(last))
    def _():
        signal(barrier, (n_clump - 1, n_group - 1))

    for k in (0, 10, 11, *range(1, 10)):
        loads[k].start()

    below = my_slab + (my_row + 1) * (my_side + 1) - 1
    due = jnp.where(keeps, below * inner_group, below + 1)

    @pl.when((due > 0) | last)
    def _():
        pl.semaphore_wait(barrier, jnp.where(last, n - 1, due))


    @pl.when(keeps)
    def _():
        def tell_column(o, device):
            for core in range(inner_group):
                signal(column.at[o], (device[0], device[1] - my_core + core))

        def tell_plane(block, device):
            for core in range(inner_group):
                signal(known.at[0], (device[0], device[1] - my_core + core))

        when_slabs(tell_column, behind, up_slab)
        when_places(tell_plane, behind, up_row, up_side)

    @pl.when(last)
    def _():
        each_other(lambda block, device: signal(known.at[1], device), ahead_of)

    table_rows = pl.ds(0, nv + 1)
    loads[10].wait()
    loads[11].wait()

    def share(block, device):
        into = tables.at[block * inner_group + my_core, table_rows]
        remote(own.at[table_rows], into, 0, keeper_of(device))

    def share_down(block, o, i):
        @pl.when((my_row >= o) & (my_side >= i))
        def _():
            back = ((inner_clump - o) % inner_clump) * outer_group + (outer_group - i) % outer_group
            share(back, place(behind, o, i, 0, 0))

    offsets(share_down, inner_clump, outer_group, far_first=True)

    @pl.when(jnp.logical_not(keeps))
    def _():
        share(0, (my_clump, my_group))

    loads[0].wait()
    target = target_ref[...]
    owner, local = split_by(target, cells)
    owner_b = jnp.broadcast_to(owner.astype(F32), (cells, cells))
    same = owner_b == owner_b.T
    earlier = iota((cells, cells), 0) < iota((cells, cells), 1)
    rank = jnp.sum(jnp.where(same & earlier, 1.0, 0.0), axis=0, keepdims=True).astype(jnp.int32)
    to_clump, to_group = split_by(owner, n_group)
    to_slab, to_row = split_by(to_clump, inner_clump)
    to_side, to_core = split_by(to_group, inner_group)
    table = behind(my_row, to_row, inner_clump) * outer_group
    table = table + behind(my_side, to_side, outer_group)
    entry = table * inner_group + to_core
    slab = behind(to_slab, my_slab, outer_clump)
    wanted = (local + 1).astype(F32)
    asks = jnp.where(iota((outer_clump, cells), 0) == slab, wanted, 0.0).astype(BF16)
    ask_rows = dot_nt(asks, onehot(iota((128, cells), 0) == entry * slots + rank))
    for k in range(outer_clump):
        ask[k, 0:1, :] = ask_rows[k : k + 1]
    one_row = pl.ds(0, 1)

    def request(step, device):
        into = asked.at[step * inner_group + my_core, one_row]
        remote(ask.at[step, one_row], into, 1, keeper_of(device))

    @pl.when(jnp.logical_not(keeps))
    def _():
        request(0, (my_clump, my_group))

    def request_down(o):
        @pl.when(my_slab >= o)
        def _():
            request(outer_clump - o, place(behind, 0, 0, o, 0))

    slabs(request_down)

    frac = frac_ref[...]
    block = behind(to_row, my_row, inner_clump) * outer_group
    block = (block + behind(to_side, my_side, outer_group)) * outer_clump + slab
    block = (block * inner_group + behind(to_core, my_core, inner_group)) * stride
    part, line = split_by(rank, half)
    slot_of = onehot(iota((2 * rows, cells), 0) == part * rows + block + line)
    asks = jnp.where(iota((rows, cells), 0) == block, wanted, 0.0).astype(BF16)
    id_rows = dot_nt(asks, onehot(iota((128, cells), 0) == rank))
    in_stride = split_by(iota((rows, 128), 0), stride)[1]
    note[...] = jnp.where(in_stride == 1, jnp.broadcast_to(frac, (rows, cells)), id_rows)
    noted[0:2, :] = note[0:2, :]

    def lines_of(block, count):
        start = block * stride
        return pl.ds(start if isinstance(start, int) else pl.multiple_of(start, stride), count)

    def give_note(block, device):
        its = lines_of(block, 2)
        remote(note.at[its], noted.at[its], 4, device)

    @pl.when(last_place & last_plane)
    def _():
        @pl.when(jnp.logical_not(last))
        def _():
            pl.semaphore_wait(known.at[1], 1)

        each_other(give_note, ahead_of)


    for load in loads[1:10]:
        load.wait()
    lu_hi, lu_lo = halves(lwt_ref[...])
    lu_rows = rows_of([lu_hi, lu_lo, lgrid_ref[...]], 16)
    lu_of = onehot(iota((lus, cols), 0) == clu_ref[...])
    col_vals = dot(lu_rows, lu_of)
    col_w = cwt_ref[...] * (col_vals[0:1] + col_vals[1:2])

    c_hi, c_lo = halves(col_w)
    col_rows = rows_of([c_hi, c_lo, col_vals[2:3]], 16)
    col_of = onehot(iota((cols, patches), 0) == pcol_ref[...])
    patch_vals = dot(col_rows, col_of)
    alive = jnp.where(iota((1, patches), 1) < count_ref[0], 1.0, 0.0)
    weight = alive * pwt_ref[...] * (patch_vals[0:1] + patch_vals[1:2])
    home = patch_vals[2:3].astype(jnp.int32)
    home_of = onehot(iota((cells, patches), 0) == home)

    scales = scale_ref[...]
    t1 = scales.astype(BF16).astype(F32)
    t2 = (scales - t1).astype(BF16).astype(F32)
    t3 = scales - t1 - t2
    pad = 128 - 3 * types
    stacked = jnp.concatenate([t1, t2, t3, jnp.zeros((pad, nv), F32)], axis=0)
    stacked = jnp.concatenate([stacked, jnp.zeros((128, 128 - nv), F32)], axis=1)
    scale_t = stacked.T[:nv].astype(BF16)
    kind = iota((128, patches), 0)
    type_of = onehot(
        (kind == pft_ref[...])
        | (kind == pft_ref[...] + types)
        | (kind == pft_ref[...] + 2 * types)
    )
    scaled = flux_ref[...] * dot(scale_t, type_of)

    x_hi, x_lo = halves(scaled * weight)
    w_hi, w_lo = halves(weight)
    sums = dot_nt(
        jnp.concatenate([x_hi, x_lo, rows_of([w_hi, w_lo], 16)], axis=0), home_of
    )
    num = sums[:nv] + sums[nv : 2 * nv]
    den = sums[2 * nv : 2 * nv + 1] + sums[2 * nv + 1 : 2 * nv + 2]
    mean = num / jnp.maximum(den, 1.0)

    send[...] = pack(slot_of, mean)
    recv[0:half, :] = send[0:half, :]
    later = (up_row + 1) * (up_side + 1) - 1

    @pl.when(later > 0)
    def _():
        pl.semaphore_wait(known.at[0], later)

    def share_rest(block, o, i):
        row, side = ahead_of(my_row, o, inner_clump), ahead_of(my_side, i, outer_group)

        @pl.when((row > my_row) | (side > my_side))
        def _():
            share(block, place(ahead_of, o, i, 0, 0))

    offsets(share_rest, inner_clump, outer_group)

    def request_up(o):
        @pl.when(up_slab >= o)
        def _():
            pl.semaphore_wait(column.at[o], 1)
            request(o, place(ahead_of, 0, 0, o, 0))

    slabs(request_up)

    @pl.when(jnp.logical_not(last_place & last_plane))
    def _():
        pl.semaphore_wait(known.at[1], 1)
        each_other(give_note, ahead_of)

    def give(block, device):
        its = lines_of(block, half)
        remote(send.at[its], recv.at[its], 2, device)

    each_other(give, ahead_of)

    @pl.when(keeps)
    def _():
        wait(tables.at[pl.ds(0, sharers - 1), table_rows], recv_sem.at[0])
        held = [own if t == keeper else tables.at[t] for t in range(sharers)]
        held = [(1.0 - x[nv : nv + 1, :]) * x[0:nv, :] for x in held]
        held = [wide(held[2 * p], held[2 * p + 1]) for p in range(pairs)]

        asked[keeper, 0:1, :] = ask[0, 0:1, :]
        wait(asked.at[pl.ds(0, askers - 1), one_row], recv_sem.at[1])
        told = jnp.broadcast_to(asked[:, 0:1, :], (askers, slots, 128)).reshape(askers * slots, 128)
        lane_less = iota((askers * slots, 128), 1) - split_by(iota((askers * slots, 128), 0), slots)[1]
        spread = [jnp.where(lane_less == t * slots, told, 0.0) for t in range(sharers)]
        ids = dot(jnp.concatenate(spread, axis=0).astype(BF16), jnp.ones((128, cells), BF16))
        held_of = onehot(ids == (iota(ids.shape, 1) + 1).astype(F32))
        for p in range(pairs):
            one, two = 2 * p * askers * slots, (2 * p + 1) * askers * slots
            packed = pack_wide(held_of[one : two + askers * slots], held[p])
            reply[:, p * slots : (p + 1) * slots, :] = packed.reshape(askers, slots, 128)

        def respond(block, o, i):
            clump, group = place(behind, 0, 0, o, 0)
            remote(reply.at[block], back.at[o], 3, (clump, group - my_core + i))

        if outer_clump <= 8:
            for o in range(outer_clump - 1, -1, -1):
                for i in range(inner_group):
                    if o or i < keeper:
                        respond(o * inner_group + i, o, i)
        else:
            for i in range(keeper):
                respond(i, 0, i)

            @pl.loop(1, outer_clump)
            def _(o):
                for i in range(inner_group):
                    respond(o * inner_group + i, o, i)

        back[0] = reply[keeper]

    other = (1.0 - frac) * field_ref[...]
    pair, side = split_by(entry, 2)
    answers = outer_clump * pairs * slots
    spot = side * answers + (slab * pairs + pair) * slots + rank
    answer_of = onehot(iota((2 * answers, cells), 0) == spot)
    patch_of = (dot(answer_of, home_of) * alive).astype(BF16)

    flat = pl.ds(0, (n - 1) * half)
    keeps_or_not = ((keeps, 1), (jnp.logical_not(keeps), 0))
    for which, first in keeps_or_not:

        @pl.when(which)
        def _(first=first):
            wait(tables.at[pl.ds(0, places - first), table_rows], send_sem.at[0])
            wait(ask.at[pl.ds(0, outer_clump - first), one_row], send_sem.at[1])

    wait(send.at[flat], send_sem.at[2])
    wait(note.at[pl.ds(0, (n - 1) * 2)], send_sem.at[4])
    wait(noted.at[pl.ds(0, (n - 1) * 2)], recv_sem.at[4])
    lane = iota((2 * rows, 128), 0)
    lane_part = jnp.where(lane >= rows, 1, 0)
    lane_line = split_by(lane - lane_part * rows, stride)[1]
    its_lane = (lane_line < half) & (
        iota((2 * rows, 128), 1) == lane_part * half + lane_line
    )
    told = jnp.where(in_stride < 2, noted[...], 0.0)
    ids_of = jnp.broadcast_to(told.reshape(n, stride, 128)[:, 0:1, :], (n, stride, 128)).reshape(rows, 128)
    spread = jnp.where(its_lane, jnp.concatenate([ids_of, ids_of], axis=0), 0.0).astype(BF16)
    ids = dot(spread, jnp.ones((128, cells), BF16))
    owned_of = onehot(ids == (iota((2 * rows, cells), 1) + 1).astype(F32))

    back_of = (table * outer_clump + behind(my_slab, to_slab, outer_clump)) * inner_group
    back_of = (back_of + behind(my_core, to_core, inner_group)) * stride + 1
    all_frac = select(told.T, onehot(iota((rows, cells), 0) == back_of))
    cell_frac = jnp.sum(
        jnp.where(iota((128, cells), 0) == local, all_frac, 0.0), axis=0, keepdims=True
    )
    base = alive * (scaled - select(cell_frac * mean, home_of))

    @pl.when(keeps)
    def _():
        wait(reply.at[pl.ds(0, askers - 1)], send_sem.at[3])

    wait(recv.at[flat], recv_sem.at[2])
    in_half = split_by(iota((rows, 128), 0), stride)[1] < half
    owned = select(unpack(jnp.where(in_half, recv[...], 0.0)), owned_of)
    merged_ref[...] = frac * owned + other

    for which, first in keeps_or_not:

        @pl.when(which)
        def _(first=first):
            wait(back.at[pl.ds(first, outer_clump - first)], recv_sem.at[3])

    anomaly_ref[...] = base - select(unpack(back[...].reshape(answers, 128)), patch_of)


def store_kernel(merged, anomaly, merged_out, anomaly_out, sem):
    stores = [
        pltpu.make_async_copy(merged, merged_out, sem.at[0]),
        pltpu.make_async_copy(anomaly, anomaly_out, sem.at[1]),
    ]
    for store in stores:
        store.start()
    for store in stores:
        store.wait()


def per_device(
    flux, patch_pft, patch_wt, patch_col, col_wt, col_lu, lu_wt, lu_grid, cell_target,
    patch_count, pft_scale, cpl_frac, cpl_field,
):
    n_clump = lax.axis_size("clump")
    n_group = lax.axis_size("grp")
    n = n_clump * n_group
    nv = flux.shape[2]
    patches = flux.shape[1]
    cells = cell_target.shape[1]
    inner_group = 2 if n_group % 2 == 0 else 1
    outer_group = n_group // inner_group
    inner_clump = outer_group if n_clump % outer_group == 0 else 1
    sharers = inner_clump * n_group
    outer_clump = n_clump // inner_clump
    askers = outer_clump * inner_group
    cap = max(2, 2 * cells // n)
    half = -(-cap // 2)
    slots = -(-cap // 8) * 8
    stride = -(-half // 8) * 8
    vmem = pl.BlockSpec(memory_space=pltpu.VMEM)
    hbm = pl.BlockSpec(memory_space=pltpu.HBM)
    staged = (
        cell_target, lu_wt, lu_grid, col_lu, col_wt, patch_col, patch_wt,
        pft_scale, patch_pft, flux[0].T,
    )
    inputs = (*staged, cpl_frac.reshape(1, -1), cpl_field.T)
    shapes = (
        jax.ShapeDtypeStruct((nv, cells), F32),
        jax.ShapeDtypeStruct((nv, patches), F32),
    )
    results = pl.pallas_call(
        functools.partial(
            kernel, n_clump, n_group, inner_clump, inner_group, cap, slots, half, stride
        ),
        out_shape=tuple(pltpu.VMEM(x.shape, x.dtype) for x in shapes),
        in_specs=[pl.BlockSpec(memory_space=pltpu.SMEM)] + [hbm] * INPUTS,
        out_specs=(vmem, vmem),
        scratch_shapes=[
            pltpu.VMEM((sharers, -(-(nv + 1) // 8) * 8, cells), F32),
            pltpu.VMEM((-(-(nv + 1) // 8) * 8, cells), F32),
            pltpu.VMEM((outer_clump, 8, 128), F32),
            pltpu.VMEM((askers, 8, 128), F32),
            pltpu.VMEM((n * stride, 128), F32),
            pltpu.VMEM((n * stride, 128), F32),
            pltpu.VMEM((askers, sharers // 2 * slots, 128), F32),
            pltpu.VMEM((outer_clump, sharers // 2 * slots, 128), F32),
            pltpu.VMEM((n * stride, 128), F32),
            pltpu.VMEM((n * stride, 128), F32),
            pltpu.SemaphoreType.DMA((5,)),
            pltpu.SemaphoreType.DMA((5,)),
            pltpu.SemaphoreType.DMA((INPUTS,)),
            pltpu.SemaphoreType.REGULAR((2,)),
            pltpu.SemaphoreType.REGULAR((outer_clump,)),
        ]
        + [pltpu.VMEM(x.shape, x.dtype) for x in staged],
        compiler_params=pltpu.CompilerParams(
            collective_id=0, has_side_effects=True, vmem_limit_bytes=48 * 1024 * 1024
        ),
    )(patch_count, *[pltpu.with_memory_space_constraint(x, pltpu.HBM) for x in inputs])
    merged, anomaly = pl.pallas_call(
        store_kernel,
        out_shape=shapes,
        in_specs=[vmem, vmem],
        out_specs=(hbm, hbm),
        scratch_shapes=[pltpu.SemaphoreType.DMA((2,))],
        compiler_params=pltpu.CompilerParams(vmem_limit_bytes=4 * 1024 * 1024),
    )(*results)
    return merged.T, anomaly.T[None]


def solution(mesh):
    split = P(("clump", "grp"))
    return jax.shard_map(
        per_device,
        mesh=mesh,
        in_specs=(split,) * 10 + (P(),) + (split,) * 2,
        out_specs=(split, split),
        check_vma=False,
    )
```

```python
import functools

import jax
import jax.numpy as jnp
from jax import lax
from jax.experimental import pallas as pl
from jax.experimental.pallas import tpu as pltpu
from jax.sharding import PartitionSpec as P

MESH = pl.DeviceIdType.MESH
F32 = jnp.float32
BF16 = jnp.bfloat16
INPUTS = 12


def iota(shape, dim):
    return lax.broadcasted_iota(jnp.int32, shape, dim)


def onehot(mask):
    return jnp.where(mask, 1.0, 0.0).astype(BF16)


def halves(x):
    high = x.astype(BF16)
    return high, (x - high.astype(F32)).astype(BF16)


def dot(a, b):
    return jnp.dot(a, b, preferred_element_type=F32)


def dot_nt(a, b):
    return lax.dot_general(a, b, (((1,), (1,)), ((), ())), preferred_element_type=F32)


def rows_of(rows, total):
    n = rows[0].shape[1]
    at = iota((total, n), 0)
    out = jnp.zeros((total, n), F32)
    for k, row in enumerate(rows):
        out = jnp.where(at == k, jnp.broadcast_to(row.astype(F32), (total, n)), out)
    return out.astype(BF16)


def split_by(x, size):
    if size & (size - 1) == 0:
        return lax.shift_right_logical(x, jnp.int32(size.bit_length() - 1)), x & (size - 1)
    return x // size, x % size


def select(table, chosen):
    high, low = halves(table)
    both = dot(jnp.concatenate([high, low], axis=0), chosen)
    return both[: table.shape[0]] + both[table.shape[0] :]


def wide(one, two):
    blank = jnp.zeros(one.shape, BF16)

    def beside(first, second):
        upper = jnp.concatenate([first, blank], axis=1)
        return jnp.concatenate([upper, jnp.concatenate([blank, second], axis=1)], axis=0)

    (high, low), (high_two, low_two) = halves(one), halves(two)
    return beside(high, high_two), beside(low, low_two)


def pack_wide(chosen, parts):
    rows = chosen.shape[0] // 2
    pair = jnp.concatenate([chosen[:rows], chosen[rows:]], axis=1)
    return dot_nt(pair, parts[0]) + dot_nt(pair, parts[1])


def pack(chosen, x):
    return pack_wide(chosen, wide(x, x))


def unpack(packed):
    turned = packed.T
    middle = turned.shape[0] // 2
    return jnp.concatenate([turned[:middle], turned[middle:]], axis=1)


def kernel(
    n_clump, n_group, inner_clump, inner_group, cap, slots, half, stride,
    *refs,
):
    count_ref, *refs = refs
    sources, refs = refs[:INPUTS], refs[INPUTS:]
    merged_ref, anomaly_ref = refs[:2]
    tables, own, ask, asked, note, noted, reply, back, send, recv = refs[2:12]
    send_sem, recv_sem, in_sem, known = refs[12:16]
    staged = refs[16:]
    (
        target_ref, lwt_ref, lgrid_ref, clu_ref, cwt_ref, pcol_ref, pwt_ref,
        scale_ref, pft_ref, flux_ref,
    ) = staged
    nv, patches = flux_ref.shape
    types = scale_ref.shape[0]
    cols = cwt_ref.shape[1]
    lus = lwt_ref.shape[1]
    cells = target_ref.shape[1]
    n = n_clump * n_group
    rows = n * stride
    outer_clump, outer_group = n_clump // inner_clump, n_group // inner_group
    places, askers = inner_clump * outer_group, outer_clump * inner_group
    sharers = places * inner_group
    pairs = sharers // 2
    field_ref, frac_ref = own.at[pl.ds(0, nv)], own.at[pl.ds(nv, 1)]
    loads = [
        pltpu.make_async_copy(source, into, in_sem.at[0 if k == 0 else 2 if k < 10 else 1])
        for k, (source, into) in enumerate(zip(sources, (*staged, frac_ref, field_ref)))
    ]
    my_clump, my_group = lax.axis_index("clump"), lax.axis_index("grp")
    my_slab, my_row = lax.div(my_clump, inner_clump), lax.rem(my_clump, inner_clump)
    my_side, my_core = lax.div(my_group, inner_group), lax.rem(my_group, inner_group)
    keeper = inner_group - 1
    keeps = my_core == keeper

    def ahead_of(mine, step, size):
        there = mine + step
        return jnp.where(there >= size, there - size, there)

    def behind(mine, step, size):
        there = mine - step
        return jnp.where(there < 0, there + size, there)

    def offsets(act, outer, inner, own=False, far_first=False):
        if outer <= 8:
            steps = [(o, i) for o in range(outer) for i in range(inner) if own or o or i]
            for o, i in steps[::-1] if far_first else steps:
                act(o * inner + i, o, i)
        else:
            for i in range(0 if own else 1, inner):
                act(i, 0, i)

            @pl.loop(1, outer)
            def _(o):
                for i in range(inner):
                    act(o * inner + i, o, i)

    def place(there, row, side, slab, core):
        slab, row = there(my_slab, slab, outer_clump), there(my_row, row, inner_clump)
        side, core = there(my_side, side, outer_group), there(my_core, core, inner_group)
        return slab * inner_clump + row, side * inner_group + core

    def each_other(act, there):
        for row in range(inner_clump - 1, -1, -1):
            for side in range(outer_group - 1, -1, -1):
                t = row * outer_group + side

                def one(block, o, i, t=t, row=row, side=side):
                    act(t * askers + block, place(there, row, side, o, i))

                offsets(one, outer_clump, inner_group, own=t > 0)

    def remote(source, into, k, device):
        sent = 1 if k == 3 else 0
        pltpu.make_async_remote_copy(
            src_ref=source,
            dst_ref=into,
            send_sem=send_sem.at[sent],
            recv_sem=recv_sem.at[k],
            device_id=device,
            device_id_type=MESH,
        ).start()

    def wait(rest, sem):
        pltpu.make_async_copy(rest, rest, sem).wait()

    barrier = pltpu.get_barrier_semaphore()

    def signal(sem, device):
        pl.semaphore_signal(sem, inc=1, device_id=device, device_id_type=MESH)

    def each_place(act, there):
        def one(block, o, i):
            act(block, place(there, o, i, 0, 0))

        offsets(one, inner_clump, outer_group, far_first=True)

    def slabs(act):
        if outer_clump <= 8:
            for o in range(1, outer_clump):
                act(o)
        else:
            pl.loop(1, outer_clump)(act)

    def each_slab(act, there):
        slabs(lambda o: act(o, place(there, 0, 0, o, 0)))

    def core_of(device, core):
        return device[0], device[1] - my_core + core

    def keeper_of(device):
        return core_of(device, keeper)

    here = (my_clump, my_group)
    last_place = (my_row == inner_clump - 1) & (my_side == outer_group - 1)
    last_plane = my_slab == outer_clump - 1
    last_chip = last_place & last_plane
    last = last_chip & keeps

    def greet(step, device):
        for core in range(inner_group):
            signal(barrier, core_of(device, core))

    @pl.when(keeps)
    def _():
        each_slab(greet, ahead_of)
        each_place(greet, ahead_of)
        for core in range(keeper):
            signal(barrier, core_of(here, core))

    @pl.when(jnp.logical_not(keeps & (last_place | last_plane)))
    def _():
        signal(barrier, (n_clump - 1, n_group - 1))

    for k in (0, 10, 11, *range(1, 10)):
        loads[k].start()

    table_rows = pl.ds(0, nv + 1)

    def share(block, device):
        into = tables.at[block * inner_group + my_core, table_rows]
        remote(own.at[table_rows], into, 0, keeper_of(device))

    def enter():
        loads[10].wait()
        loads[11].wait()
        near = outer_clump + places - 2 + jnp.where(keeps, 0, 1)
        pl.semaphore_wait(barrier, jnp.where(last, n - 1, near))
        each_place(share, ahead_of)

        @pl.when(jnp.logical_not(keeps))
        def _():
            share(0, here)

        @pl.when(last)
        def _():
            each_other(lambda block, device: signal(known, device), ahead_of)

    pl.when(last_chip)(enter)
    loads[0].wait()
    target = target_ref[...]
    owner, local = split_by(target, cells)
    owner_b = jnp.broadcast_to(owner.astype(F32), (cells, cells))
    same = owner_b == owner_b.T
    earlier = iota((cells, cells), 0) < iota((cells, cells), 1)
    rank = jnp.sum(jnp.where(same & earlier, 1.0, 0.0), axis=0, keepdims=True).astype(jnp.int32)
    to_clump, to_group = split_by(owner, n_group)
    to_slab, to_row = split_by(to_clump, inner_clump)
    to_side, to_core = split_by(to_group, inner_group)
    table = behind(my_row, to_row, inner_clump) * outer_group
    table = table + behind(my_side, to_side, outer_group)
    entry = table * inner_group + to_core
    slab = behind(to_slab, my_slab, outer_clump)
    wanted = (local + 1).astype(F32)
    asks = jnp.where(iota((outer_clump, cells), 0) == slab, wanted, 0.0).astype(BF16)
    ask_rows = dot_nt(asks, onehot(iota((128, cells), 0) == entry * slots + rank))
    for k in range(outer_clump):
        ask[k, 0:1, :] = ask_rows[k : k + 1]
    one_row = pl.ds(0, 1)
    pl.when(jnp.logical_not(last_chip))(enter)

    def request(step, device):
        into = asked.at[step * inner_group + my_core, one_row]
        remote(ask.at[step, one_row], into, 1, keeper_of(device))

    @pl.when(jnp.logical_not(keeps))
    def _():
        request(0, here)

    each_slab(request, ahead_of)
    frac = frac_ref[...]
    block = behind(to_row, my_row, inner_clump) * outer_group
    block = (block + behind(to_side, my_side, outer_group)) * outer_clump + slab
    block = (block * inner_group + behind(to_core, my_core, inner_group)) * stride
    part, line = split_by(rank, half)
    slot_of = onehot(iota((2 * rows, cells), 0) == part * rows + block + line)
    asks = jnp.where(iota((rows, cells), 0) == block, wanted, 0.0).astype(BF16)
    id_rows = dot_nt(asks, onehot(iota((128, cells), 0) == rank))
    in_stride = split_by(iota((rows, 128), 0), stride)[1]
    note[...] = jnp.where(in_stride == 1, jnp.broadcast_to(frac, (rows, cells)), id_rows)
    noted[0:2, :] = note[0:2, :]

    def lines_of(block, count):
        start = block * stride
        return pl.ds(start if isinstance(start, int) else pl.multiple_of(start, stride), count)

    def give_note(block, device):
        its = lines_of(block, 2)
        remote(note.at[its], noted.at[its], 4, device)

    @pl.when(last_chip)
    def _():
        @pl.when(jnp.logical_not(last))
        def _():
            pl.semaphore_wait(known, 1)

        each_other(give_note, ahead_of)


    for load in loads[1:10]:
        load.wait()
    lu_hi, lu_lo = halves(lwt_ref[...])
    lu_rows = rows_of([lu_hi, lu_lo, lgrid_ref[...]], 16)
    lu_of = onehot(iota((lus, cols), 0) == clu_ref[...])
    col_vals = dot(lu_rows, lu_of)
    col_w = cwt_ref[...] * (col_vals[0:1] + col_vals[1:2])

    c_hi, c_lo = halves(col_w)
    col_rows = rows_of([c_hi, c_lo, col_vals[2:3]], 16)
    col_of = onehot(iota((cols, patches), 0) == pcol_ref[...])
    patch_vals = dot(col_rows, col_of)
    alive = jnp.where(iota((1, patches), 1) < count_ref[0], 1.0, 0.0)
    weight = alive * pwt_ref[...] * (patch_vals[0:1] + patch_vals[1:2])
    home = patch_vals[2:3].astype(jnp.int32)
    home_of = onehot(iota((cells, patches), 0) == home)

    scales = scale_ref[...]
    t1 = scales.astype(BF16).astype(F32)
    t2 = (scales - t1).astype(BF16).astype(F32)
    t3 = scales - t1 - t2
    pad = 128 - 3 * types
    stacked = jnp.concatenate([t1, t2, t3, jnp.zeros((pad, nv), F32)], axis=0)
    stacked = jnp.concatenate([stacked, jnp.zeros((128, 128 - nv), F32)], axis=1)
    scale_t = stacked.T[:nv].astype(BF16)
    kind = iota((128, patches), 0)
    type_of = onehot(
        (kind == pft_ref[...])
        | (kind == pft_ref[...] + types)
        | (kind == pft_ref[...] + 2 * types)
    )
    scaled = flux_ref[...] * dot(scale_t, type_of)

    x_hi, x_lo = halves(scaled * weight)
    w_hi, w_lo = halves(weight)
    sums = dot_nt(
        jnp.concatenate([x_hi, x_lo, rows_of([w_hi, w_lo], 16)], axis=0), home_of
    )
    num = sums[:nv] + sums[nv : 2 * nv]
    den = sums[2 * nv : 2 * nv + 1] + sums[2 * nv + 1 : 2 * nv + 2]
    mean = num / jnp.maximum(den, 1.0)

    send[...] = pack(slot_of, mean)
    recv[0:half, :] = send[0:half, :]
    @pl.when(jnp.logical_not(last_chip))
    def _():
        pl.semaphore_wait(known, 1)
        each_other(give_note, ahead_of)

    def give(block, device):
        its = lines_of(block, half)
        remote(send.at[its], recv.at[its], 2, device)

    each_other(give, ahead_of)

    @pl.when(keeps)
    def _():
        asked[keeper, 0:1, :] = ask[0, 0:1, :]
        wait(asked.at[pl.ds(0, askers - 1), one_row], recv_sem.at[1])
        told = jnp.broadcast_to(asked[:, 0:1, :], (askers, slots, 128)).reshape(askers * slots, 128)
        lane_less = iota((askers * slots, 128), 1) - split_by(iota((askers * slots, 128), 0), slots)[1]
        spread = [jnp.where(lane_less == t * slots, told, 0.0) for t in range(sharers)]
        ids = dot(jnp.concatenate(spread, axis=0).astype(BF16), jnp.ones((128, cells), BF16))
        held_of = onehot(ids == (iota(ids.shape, 1) + 1).astype(F32))

        wait(tables.at[pl.ds(0, sharers - 1), table_rows], recv_sem.at[0])
        held = [own if t == keeper else tables.at[t] for t in range(sharers)]
        held = [(1.0 - x[nv : nv + 1, :]) * x[0:nv, :] for x in held]
        held = [wide(held[2 * p], held[2 * p + 1]) for p in range(pairs)]
        for p in range(pairs):
            one, two = 2 * p * askers * slots, (2 * p + 1) * askers * slots
            packed = pack_wide(held_of[one : two + askers * slots], held[p])
            reply[:, p * slots : (p + 1) * slots, :] = packed.reshape(askers, slots, 128)

        def respond(block, o, i):
            clump, group = place(behind, 0, 0, o, 0)
            remote(reply.at[block], back.at[o], 3, (clump, group - my_core + i))

        if outer_clump <= 8:
            for o in range(outer_clump - 1, -1, -1):
                for i in range(inner_group):
                    if o or i < keeper:
                        respond(o * inner_group + i, o, i)
        else:
            for i in range(keeper):
                respond(i, 0, i)

            @pl.loop(1, outer_clump)
            def _(o):
                for i in range(inner_group):
                    respond(o * inner_group + i, o, i)

        back[0] = reply[keeper]

    other = (1.0 - frac) * field_ref[...]
    pair, side = split_by(entry, 2)
    answers = outer_clump * pairs * slots
    spot = side * answers + (slab * pairs + pair) * slots + rank
    answer_of = onehot(iota((2 * answers, cells), 0) == spot)
    patch_of = (dot(answer_of, home_of) * alive).astype(BF16)

    flat = pl.ds(0, (n - 1) * half)
    keeps_or_not = ((keeps, 1), (jnp.logical_not(keeps), 0))
    for which, first in keeps_or_not:

        @pl.when(which)
        def _(first=first):
            wait(tables.at[pl.ds(0, places - first), table_rows], send_sem.at[0])
            wait(ask.at[pl.ds(0, outer_clump - first), one_row], send_sem.at[0])

    wait(send.at[flat], send_sem.at[0])
    wait(note.at[pl.ds(0, (n - 1) * 2)], send_sem.at[0])
    wait(noted.at[pl.ds(0, (n - 1) * 2)], recv_sem.at[4])
    lane = iota((2 * rows, 128), 0)
    lane_part = jnp.where(lane >= rows, 1, 0)
    lane_line = split_by(lane - lane_part * rows, stride)[1]
    its_lane = (lane_line < half) & (
        iota((2 * rows, 128), 1) == lane_part * half + lane_line
    )
    told = jnp.where(in_stride < 2, noted[...], 0.0)
    ids_of = jnp.broadcast_to(told.reshape(n, stride, 128)[:, 0:1, :], (n, stride, 128)).reshape(rows, 128)
    spread = jnp.where(its_lane, jnp.concatenate([ids_of, ids_of], axis=0), 0.0).astype(BF16)
    ids = dot(spread, jnp.ones((128, cells), BF16))
    owned_of = onehot(ids == (iota((2 * rows, cells), 1) + 1).astype(F32))

    back_of = (table * outer_clump + behind(my_slab, to_slab, outer_clump)) * inner_group
    back_of = (back_of + behind(my_core, to_core, inner_group)) * stride + 1
    all_frac = select(told.T, onehot(iota((rows, cells), 0) == back_of))
    cell_frac = jnp.sum(
        jnp.where(iota((128, cells), 0) == local, all_frac, 0.0), axis=0, keepdims=True
    )
    base = alive * (scaled - select(cell_frac * mean, home_of))

    @pl.when(keeps)
    def _():
        wait(reply.at[pl.ds(0, askers - 1)], send_sem.at[1])

    wait(recv.at[flat], recv_sem.at[2])
    in_half = split_by(iota((rows, 128), 0), stride)[1] < half
    owned = select(unpack(jnp.where(in_half, recv[...], 0.0)), owned_of)
    merged_ref[...] = frac * owned + other

    for which, first in keeps_or_not:

        @pl.when(which)
        def _(first=first):
            wait(back.at[pl.ds(first, outer_clump - first)], recv_sem.at[3])

    anomaly_ref[...] = base - select(unpack(back[...].reshape(answers, 128)), patch_of)


def store_kernel(merged, anomaly, merged_out, anomaly_out, sem):
    stores = [
        pltpu.make_async_copy(merged, merged_out, sem.at[0]),
        pltpu.make_async_copy(anomaly, anomaly_out, sem.at[1]),
    ]
    for store in stores:
        store.start()
    for store in stores:
        store.wait()


def per_device(
    flux, patch_pft, patch_wt, patch_col, col_wt, col_lu, lu_wt, lu_grid, cell_target,
    patch_count, pft_scale, cpl_frac, cpl_field,
):
    n_clump = lax.axis_size("clump")
    n_group = lax.axis_size("grp")
    n = n_clump * n_group
    nv = flux.shape[2]
    patches = flux.shape[1]
    cells = cell_target.shape[1]
    inner_group = 2 if n_group % 2 == 0 else 1
    outer_group = n_group // inner_group
    inner_clump = outer_group if n_clump % outer_group == 0 else 1
    sharers = inner_clump * n_group
    outer_clump = n_clump // inner_clump
    askers = outer_clump * inner_group
    cap = max(2, 2 * cells // n)
    half = -(-cap // 2)
    slots = -(-cap // 8) * 8
    stride = -(-half // 8) * 8
    vmem = pl.BlockSpec(memory_space=pltpu.VMEM)
    hbm = pl.BlockSpec(memory_space=pltpu.HBM)
    staged = (
        cell_target, lu_wt, lu_grid, col_lu, col_wt, patch_col, patch_wt,
        pft_scale, patch_pft, flux[0].T,
    )
    inputs = (*staged, cpl_frac.reshape(1, -1), cpl_field.T)
    shapes = (
        jax.ShapeDtypeStruct((nv, cells), F32),
        jax.ShapeDtypeStruct((nv, patches), F32),
    )
    results = pl.pallas_call(
        functools.partial(
            kernel, n_clump, n_group, inner_clump, inner_group, cap, slots, half, stride
        ),
        out_shape=tuple(pltpu.VMEM(x.shape, x.dtype) for x in shapes),
        in_specs=[pl.BlockSpec(memory_space=pltpu.SMEM)] + [hbm] * INPUTS,
        out_specs=(vmem, vmem),
        scratch_shapes=[
            pltpu.VMEM((sharers, -(-(nv + 1) // 8) * 8, cells), F32),
            pltpu.VMEM((-(-(nv + 1) // 8) * 8, cells), F32),
            pltpu.VMEM((outer_clump, 8, 128), F32),
            pltpu.VMEM((askers, 8, 128), F32),
            pltpu.VMEM((n * stride, 128), F32),
            pltpu.VMEM((n * stride, 128), F32),
            pltpu.VMEM((askers, sharers // 2 * slots, 128), F32),
            pltpu.VMEM((outer_clump, sharers // 2 * slots, 128), F32),
            pltpu.VMEM((n * stride, 128), F32),
            pltpu.VMEM((n * stride, 128), F32),
            pltpu.SemaphoreType.DMA((2,)),
            pltpu.SemaphoreType.DMA((5,)),
            pltpu.SemaphoreType.DMA((3,)),
            pltpu.SemaphoreType.REGULAR,
        ]
        + [pltpu.VMEM(x.shape, x.dtype) for x in staged],
        compiler_params=pltpu.CompilerParams(
            collective_id=0, has_side_effects=True, vmem_limit_bytes=48 * 1024 * 1024
        ),
    )(patch_count, *[pltpu.with_memory_space_constraint(x, pltpu.HBM) for x in inputs])
    merged, anomaly = pl.pallas_call(
        store_kernel,
        out_shape=shapes,
        in_specs=[vmem, vmem],
        out_specs=(hbm, hbm),
        scratch_shapes=[pltpu.SemaphoreType.DMA((2,))],
        compiler_params=pltpu.CompilerParams(vmem_limit_bytes=4 * 1024 * 1024),
    )(*results)
    return merged.T, anomaly.T[None]


def solution(mesh):
    split = P(("clump", "grp"))
    return jax.shard_map(
        per_device,
        mesh=mesh,
        in_specs=(split,) * 10 + (P(),) + (split,) * 2,
        out_specs=(split, split),
        check_vma=False,
    )
```

```python
import functools

import jax
import jax.numpy as jnp
from jax import lax
from jax.experimental import pallas as pl
from jax.experimental.pallas import tpu as pltpu
from jax.sharding import PartitionSpec as P

MESH = pl.DeviceIdType.MESH
F32 = jnp.float32
BF16 = jnp.bfloat16
INPUTS = 12


def iota(shape, dim):
    return lax.broadcasted_iota(jnp.int32, shape, dim)


def onehot(mask):
    return jnp.where(mask, 1.0, 0.0).astype(BF16)


def halves(x):
    high = x.astype(BF16)
    return high, (x - high.astype(F32)).astype(BF16)


def dot(a, b):
    return jnp.dot(a, b, preferred_element_type=F32)


def dot_nt(a, b):
    return lax.dot_general(a, b, (((1,), (1,)), ((), ())), preferred_element_type=F32)


def rows_of(rows, total):
    n = rows[0].shape[1]
    at = iota((total, n), 0)
    out = jnp.zeros((total, n), F32)
    for k, row in enumerate(rows):
        out = jnp.where(at == k, jnp.broadcast_to(row.astype(F32), (total, n)), out)
    return out.astype(BF16)


def split_by(x, size):
    if size & (size - 1) == 0:
        return lax.shift_right_logical(x, jnp.int32(size.bit_length() - 1)), x & (size - 1)
    return x // size, x % size


def select(table, chosen):
    high, low = halves(table)
    both = dot(jnp.concatenate([high, low], axis=0), chosen)
    return both[: table.shape[0]] + both[table.shape[0] :]


def wide(one, two):
    blank = jnp.zeros(one.shape, BF16)

    def beside(first, second):
        upper = jnp.concatenate([first, blank], axis=1)
        return jnp.concatenate([upper, jnp.concatenate([blank, second], axis=1)], axis=0)

    (high, low), (high_two, low_two) = halves(one), halves(two)
    return beside(high, high_two), beside(low, low_two)


def pack_wide(chosen, parts):
    rows = chosen.shape[0] // 2
    pair = jnp.concatenate([chosen[:rows], chosen[rows:]], axis=1)
    return dot_nt(pair, parts[0]) + dot_nt(pair, parts[1])


def pack(chosen, x):
    return pack_wide(chosen, wide(x, x))


def unpack(packed):
    turned = packed.T
    middle = turned.shape[0] // 2
    return jnp.concatenate([turned[:middle], turned[middle:]], axis=1)


def kernel(
    n_clump, n_group, inner_clump, inner_group, cap, slots, half, stride,
    *refs,
):
    count_ref, *refs = refs
    sources, refs = refs[:INPUTS], refs[INPUTS:]
    merged_ref, base_ref, patch_of_ref, answers_ref = refs[:4]
    tables, own, ask, asked, note, noted, reply, back, send, recv = refs[4:14]
    send_sem, recv_sem, in_sem, known = refs[14:18]
    staged = refs[18:]
    (
        target_ref, lwt_ref, lgrid_ref, clu_ref, cwt_ref, pcol_ref, pwt_ref,
        scale_ref, pft_ref, flux_ref,
    ) = staged
    nv, patches = flux_ref.shape
    types = scale_ref.shape[0]
    cols = cwt_ref.shape[1]
    lus = lwt_ref.shape[1]
    cells = target_ref.shape[1]
    n = n_clump * n_group
    rows = n * stride
    outer_clump, outer_group = n_clump // inner_clump, n_group // inner_group
    places, askers = inner_clump * outer_group, outer_clump * inner_group
    sharers = places * inner_group
    pairs = sharers // 2
    field_ref, frac_ref = own.at[pl.ds(0, nv)], own.at[pl.ds(nv, 1)]
    loads = [
        pltpu.make_async_copy(source, into, in_sem.at[0 if k == 0 else 2 if k < 10 else 1])
        for k, (source, into) in enumerate(zip(sources, (*staged, frac_ref, field_ref)))
    ]
    my_clump, my_group = lax.axis_index("clump"), lax.axis_index("grp")
    my_slab, my_row = lax.div(my_clump, inner_clump), lax.rem(my_clump, inner_clump)
    my_side, my_core = lax.div(my_group, inner_group), lax.rem(my_group, inner_group)
    keeper = inner_group - 1
    keeps = my_core == keeper

    def ahead_of(mine, step, size):
        there = mine + step
        return jnp.where(there >= size, there - size, there)

    def behind(mine, step, size):
        there = mine - step
        return jnp.where(there < 0, there + size, there)

    def offsets(act, outer, inner, own=False, far_first=False):
        if outer <= 8:
            steps = [(o, i) for o in range(outer) for i in range(inner) if own or o or i]
            for o, i in steps[::-1] if far_first else steps:
                act(o * inner + i, o, i)
        else:
            for i in range(0 if own else 1, inner):
                act(i, 0, i)

            @pl.loop(1, outer)
            def _(o):
                for i in range(inner):
                    act(o * inner + i, o, i)

    def place(there, row, side, slab, core):
        slab, row = there(my_slab, slab, outer_clump), there(my_row, row, inner_clump)
        side, core = there(my_side, side, outer_group), there(my_core, core, inner_group)
        return slab * inner_clump + row, side * inner_group + core

    def each_other(act, there):
        for row in range(inner_clump - 1, -1, -1):
            for side in range(outer_group - 1, -1, -1):
                t = row * outer_group + side

                def one(block, o, i, t=t, row=row, side=side):
                    act(t * askers + block, place(there, row, side, o, i))

                offsets(one, outer_clump, inner_group, own=t > 0)

    def remote(source, into, k, device):
        sent = 1 if k == 3 else 0
        pltpu.make_async_remote_copy(
            src_ref=source,
            dst_ref=into,
            send_sem=send_sem.at[sent],
            recv_sem=recv_sem.at[k],
            device_id=device,
            device_id_type=MESH,
        ).start()

    def wait(rest, sem):
        pltpu.make_async_copy(rest, rest, sem).wait()

    barrier = pltpu.get_barrier_semaphore()

    def signal(sem, device):
        pl.semaphore_signal(sem, inc=1, device_id=device, device_id_type=MESH)

    def each_place(act, there):
        def one(block, o, i):
            act(block, place(there, o, i, 0, 0))

        offsets(one, inner_clump, outer_group, far_first=True)

    def slabs(act):
        if outer_clump <= 8:
            for o in range(1, outer_clump):
                act(o)
        else:
            pl.loop(1, outer_clump)(act)

    def each_slab(act, there):
        slabs(lambda o: act(o, place(there, 0, 0, o, 0)))

    def core_of(device, core):
        return device[0], device[1] - my_core + core

    def keeper_of(device):
        return core_of(device, keeper)

    here = (my_clump, my_group)
    last_place = (my_row == inner_clump - 1) & (my_side == outer_group - 1)
    last_plane = my_slab == outer_clump - 1
    last_chip = last_place & last_plane
    last = last_chip & keeps

    def greet(step, device):
        for core in range(inner_group):
            signal(barrier, core_of(device, core))

    @pl.when(keeps)
    def _():
        each_slab(greet, ahead_of)
        each_place(greet, ahead_of)
        for core in range(keeper):
            signal(barrier, core_of(here, core))

    @pl.when(jnp.logical_not(keeps & (last_place | last_plane)))
    def _():
        signal(barrier, (n_clump - 1, n_group - 1))

    for k in (0, 10, 11, *range(1, 10)):
        loads[k].start()

    table_rows = pl.ds(0, nv + 1)

    def share(block, device):
        into = tables.at[block * inner_group + my_core, table_rows]
        remote(own.at[table_rows], into, 0, keeper_of(device))

    def enter():
        loads[10].wait()
        loads[11].wait()
        near = outer_clump + places - 2 + jnp.where(keeps, 0, 1)
        pl.semaphore_wait(barrier, jnp.where(last, n - 1, near))
        each_place(share, ahead_of)

        @pl.when(jnp.logical_not(keeps))
        def _():
            share(0, here)

        @pl.when(last)
        def _():
            each_other(lambda block, device: signal(known, device), ahead_of)

    pl.when(last_chip)(enter)
    loads[0].wait()
    target = target_ref[...]
    owner, local = split_by(target, cells)
    owner_b = jnp.broadcast_to(owner.astype(F32), (cells, cells))
    same = owner_b == owner_b.T
    earlier = iota((cells, cells), 0) < iota((cells, cells), 1)
    rank = jnp.sum(jnp.where(same & earlier, 1.0, 0.0), axis=0, keepdims=True).astype(jnp.int32)
    to_clump, to_group = split_by(owner, n_group)
    to_slab, to_row = split_by(to_clump, inner_clump)
    to_side, to_core = split_by(to_group, inner_group)
    table = behind(my_row, to_row, inner_clump) * outer_group
    table = table + behind(my_side, to_side, outer_group)
    entry = table * inner_group + to_core
    slab = behind(to_slab, my_slab, outer_clump)
    wanted = (local + 1).astype(F32)
    asks = jnp.where(iota((outer_clump, cells), 0) == slab, wanted, 0.0).astype(BF16)
    ask_rows = dot_nt(asks, onehot(iota((128, cells), 0) == entry * slots + rank))
    for k in range(outer_clump):
        ask[k, 0:1, :] = ask_rows[k : k + 1]
    one_row = pl.ds(0, 1)
    pl.when(jnp.logical_not(last_chip))(enter)

    def request(step, device):
        into = asked.at[step * inner_group + my_core, one_row]
        remote(ask.at[step, one_row], into, 1, keeper_of(device))

    @pl.when(jnp.logical_not(keeps))
    def _():
        request(0, here)

    each_slab(request, ahead_of)
    frac = frac_ref[...]
    block = behind(to_row, my_row, inner_clump) * outer_group
    block = (block + behind(to_side, my_side, outer_group)) * outer_clump + slab
    block = (block * inner_group + behind(to_core, my_core, inner_group)) * stride
    part, line = split_by(rank, half)
    slot_of = onehot(iota((2 * rows, cells), 0) == part * rows + block + line)
    asks = jnp.where(iota((rows, cells), 0) == block, wanted, 0.0).astype(BF16)
    id_rows = dot_nt(asks, onehot(iota((128, cells), 0) == rank))
    in_stride = split_by(iota((rows, 128), 0), stride)[1]
    note[...] = jnp.where(in_stride == 1, jnp.broadcast_to(frac, (rows, cells)), id_rows)
    noted[0:2, :] = note[0:2, :]

    def lines_of(block, count):
        start = block * stride
        return pl.ds(start if isinstance(start, int) else pl.multiple_of(start, stride), count)

    def give_note(block, device):
        its = lines_of(block, 2)
        remote(note.at[its], noted.at[its], 4, device)

    @pl.when(last_chip)
    def _():
        @pl.when(jnp.logical_not(last))
        def _():
            pl.semaphore_wait(known, 1)

        each_other(give_note, ahead_of)


    for load in loads[1:10]:
        load.wait()
    lu_hi, lu_lo = halves(lwt_ref[...])
    lu_rows = rows_of([lu_hi, lu_lo, lgrid_ref[...]], 16)
    lu_of = onehot(iota((lus, cols), 0) == clu_ref[...])
    col_vals = dot(lu_rows, lu_of)
    col_w = cwt_ref[...] * (col_vals[0:1] + col_vals[1:2])

    c_hi, c_lo = halves(col_w)
    col_rows = rows_of([c_hi, c_lo, col_vals[2:3]], 16)
    col_of = onehot(iota((cols, patches), 0) == pcol_ref[...])
    patch_vals = dot(col_rows, col_of)
    alive = jnp.where(iota((1, patches), 1) < count_ref[0], 1.0, 0.0)
    weight = alive * pwt_ref[...] * (patch_vals[0:1] + patch_vals[1:2])
    home = patch_vals[2:3].astype(jnp.int32)
    home_of = onehot(iota((cells, patches), 0) == home)

    scales = scale_ref[...]
    t1 = scales.astype(BF16).astype(F32)
    t2 = (scales - t1).astype(BF16).astype(F32)
    t3 = scales - t1 - t2
    pad = 128 - 3 * types
    stacked = jnp.concatenate([t1, t2, t3, jnp.zeros((pad, nv), F32)], axis=0)
    stacked = jnp.concatenate([stacked, jnp.zeros((128, 128 - nv), F32)], axis=1)
    scale_t = stacked.T[:nv].astype(BF16)
    kind = iota((128, patches), 0)
    type_of = onehot(
        (kind == pft_ref[...])
        | (kind == pft_ref[...] + types)
        | (kind == pft_ref[...] + 2 * types)
    )
    scaled = flux_ref[...] * dot(scale_t, type_of)

    x_hi, x_lo = halves(scaled * weight)
    w_hi, w_lo = halves(weight)
    sums = dot_nt(
        jnp.concatenate([x_hi, x_lo, rows_of([w_hi, w_lo], 16)], axis=0), home_of
    )
    num = sums[:nv] + sums[nv : 2 * nv]
    den = sums[2 * nv : 2 * nv + 1] + sums[2 * nv + 1 : 2 * nv + 2]
    mean = num / jnp.maximum(den, 1.0)

    send[...] = pack(slot_of, mean)
    recv[0:half, :] = send[0:half, :]
    @pl.when(jnp.logical_not(last_chip))
    def _():
        pl.semaphore_wait(known, 1)
        each_other(give_note, ahead_of)

    def give(block, device):
        its = lines_of(block, half)
        remote(send.at[its], recv.at[its], 2, device)

    each_other(give, ahead_of)

    @pl.when(keeps)
    def _():
        asked[keeper, 0:1, :] = ask[0, 0:1, :]
        wait(asked.at[pl.ds(0, askers - 1), one_row], recv_sem.at[1])
        told = jnp.broadcast_to(asked[:, 0:1, :], (askers, slots, 128)).reshape(askers * slots, 128)
        lane_less = iota((askers * slots, 128), 1) - split_by(iota((askers * slots, 128), 0), slots)[1]
        spread = [jnp.where(lane_less == t * slots, told, 0.0) for t in range(sharers)]
        ids = dot(jnp.concatenate(spread, axis=0).astype(BF16), jnp.ones((128, cells), BF16))
        held_of = onehot(ids == (iota(ids.shape, 1) + 1).astype(F32))

        wait(tables.at[pl.ds(0, sharers - 1), table_rows], recv_sem.at[0])
        held = [own if t == keeper else tables.at[t] for t in range(sharers)]
        held = [(1.0 - x[nv : nv + 1, :]) * x[0:nv, :] for x in held]
        held = [wide(held[2 * p], held[2 * p + 1]) for p in range(pairs)]
        for p in range(pairs):
            one, two = 2 * p * askers * slots, (2 * p + 1) * askers * slots
            packed = pack_wide(held_of[one : two + askers * slots], held[p])
            reply[:, p * slots : (p + 1) * slots, :] = packed.reshape(askers, slots, 128)

        def respond(block, o, i):
            clump, group = place(behind, 0, 0, o, 0)
            remote(reply.at[block], back.at[o], 3, (clump, group - my_core + i))

        if outer_clump <= 8:
            for o in range(outer_clump - 1, -1, -1):
                for i in range(inner_group):
                    if o or i < keeper:
                        respond(o * inner_group + i, o, i)
        else:
            for i in range(keeper):
                respond(i, 0, i)

            @pl.loop(1, outer_clump)
            def _(o):
                for i in range(inner_group):
                    respond(o * inner_group + i, o, i)

        back[0] = reply[keeper]

    other = (1.0 - frac) * field_ref[...]
    pair, side = split_by(entry, 2)
    answers = outer_clump * pairs * slots
    spot = side * answers + (slab * pairs + pair) * slots + rank
    answer_of = onehot(iota((2 * answers, cells), 0) == spot)
    patch_of_ref[...] = (dot(answer_of, home_of) * alive).astype(BF16)

    flat = pl.ds(0, (n - 1) * half)
    keeps_or_not = ((keeps, 1), (jnp.logical_not(keeps), 0))
    for which, first in keeps_or_not:

        @pl.when(which)
        def _(first=first):
            wait(tables.at[pl.ds(0, places - first), table_rows], send_sem.at[0])
            wait(ask.at[pl.ds(0, outer_clump - first), one_row], send_sem.at[0])

    wait(send.at[flat], send_sem.at[0])
    wait(note.at[pl.ds(0, (n - 1) * 2)], send_sem.at[0])
    wait(noted.at[pl.ds(0, (n - 1) * 2)], recv_sem.at[4])
    lane = iota((2 * rows, 128), 0)
    lane_part = jnp.where(lane >= rows, 1, 0)
    lane_line = split_by(lane - lane_part * rows, stride)[1]
    its_lane = (lane_line < half) & (
        iota((2 * rows, 128), 1) == lane_part * half + lane_line
    )
    told = jnp.where(in_stride < 2, noted[...], 0.0)
    ids_of = jnp.broadcast_to(told.reshape(n, stride, 128)[:, 0:1, :], (n, stride, 128)).reshape(rows, 128)
    spread = jnp.where(its_lane, jnp.concatenate([ids_of, ids_of], axis=0), 0.0).astype(BF16)
    ids = dot(spread, jnp.ones((128, cells), BF16))
    owned_of = onehot(ids == (iota((2 * rows, cells), 1) + 1).astype(F32))

    back_of = (table * outer_clump + behind(my_slab, to_slab, outer_clump)) * inner_group
    back_of = (back_of + behind(my_core, to_core, inner_group)) * stride + 1
    all_frac = select(told.T, onehot(iota((rows, cells), 0) == back_of))
    cell_frac = jnp.sum(
        jnp.where(iota((128, cells), 0) == local, all_frac, 0.0), axis=0, keepdims=True
    )
    base_ref[...] = alive * (scaled - select(cell_frac * mean, home_of))

    @pl.when(keeps)
    def _():
        wait(reply.at[pl.ds(0, askers - 1)], send_sem.at[1])

    wait(recv.at[flat], recv_sem.at[2])
    in_half = split_by(iota((rows, 128), 0), stride)[1] < half
    owned = select(unpack(jnp.where(in_half, recv[...], 0.0)), owned_of)
    merged_ref[...] = frac * owned + other

    for which, first in keeps_or_not:

        @pl.when(which)
        def _(first=first):
            wait(back.at[pl.ds(first, outer_clump - first)], recv_sem.at[3])

    answers_ref[...] = back[...].reshape(answers, 128)


def store_kernel(merged, base, patch_of, answers, merged_out, anomaly_out, anomaly, sem):
    chunks = anomaly.shape[0]
    width = anomaly.shape[2]
    stores = [pltpu.make_async_copy(merged, merged_out, sem.at[chunks])]
    stores[0].start()
    high, low = halves(unpack(answers[...]))
    table = jnp.concatenate([high, low], axis=0)
    for k in range(chunks):
        its = pl.ds(k * width, width)
        both = dot(table, patch_of[:, its])
        anomaly[k] = base[:, its] - (both[: high.shape[0]] + both[high.shape[0] :])
        stores.append(pltpu.make_async_copy(anomaly.at[k], anomaly_out.at[:, its], sem.at[k]))
        stores[-1].start()
    for store in stores:
        store.wait()


def per_device(
    flux, patch_pft, patch_wt, patch_col, col_wt, col_lu, lu_wt, lu_grid, cell_target,
    patch_count, pft_scale, cpl_frac, cpl_field,
):
    n_clump = lax.axis_size("clump")
    n_group = lax.axis_size("grp")
    n = n_clump * n_group
    nv = flux.shape[2]
    patches = flux.shape[1]
    cells = cell_target.shape[1]
    inner_group = 2 if n_group % 2 == 0 else 1
    outer_group = n_group // inner_group
    inner_clump = outer_group if n_clump % outer_group == 0 else 1
    sharers = inner_clump * n_group
    outer_clump = n_clump // inner_clump
    askers = outer_clump * inner_group
    cap = max(2, 2 * cells // n)
    half = -(-cap // 2)
    slots = -(-cap // 8) * 8
    stride = -(-half // 8) * 8
    answers = outer_clump * (sharers // 2) * slots
    chunks = 2
    vmem = pl.BlockSpec(memory_space=pltpu.VMEM)
    hbm = pl.BlockSpec(memory_space=pltpu.HBM)
    staged = (
        cell_target, lu_wt, lu_grid, col_lu, col_wt, patch_col, patch_wt,
        pft_scale, patch_pft, flux[0].T,
    )
    inputs = (*staged, cpl_frac.reshape(1, -1), cpl_field.T)
    shapes = (
        jax.ShapeDtypeStruct((nv, cells), F32),
        jax.ShapeDtypeStruct((nv, patches), F32),
    )
    results = pl.pallas_call(
        functools.partial(
            kernel, n_clump, n_group, inner_clump, inner_group, cap, slots, half, stride
        ),
        out_shape=(
            pltpu.VMEM((nv, cells), F32),
            pltpu.VMEM((nv, patches), F32),
            pltpu.VMEM((2 * answers, patches), BF16),
            pltpu.VMEM((answers, 128), F32),
        ),
        in_specs=[pl.BlockSpec(memory_space=pltpu.SMEM)] + [hbm] * INPUTS,
        out_specs=(vmem,) * 4,
        scratch_shapes=[
            pltpu.VMEM((sharers, -(-(nv + 1) // 8) * 8, cells), F32),
            pltpu.VMEM((-(-(nv + 1) // 8) * 8, cells), F32),
            pltpu.VMEM((outer_clump, 8, 128), F32),
            pltpu.VMEM((askers, 8, 128), F32),
            pltpu.VMEM((n * stride, 128), F32),
            pltpu.VMEM((n * stride, 128), F32),
            pltpu.VMEM((askers, sharers // 2 * slots, 128), F32),
            pltpu.VMEM((outer_clump, sharers // 2 * slots, 128), F32),
            pltpu.VMEM((n * stride, 128), F32),
            pltpu.VMEM((n * stride, 128), F32),
            pltpu.SemaphoreType.DMA((2,)),
            pltpu.SemaphoreType.DMA((5,)),
            pltpu.SemaphoreType.DMA((3,)),
            pltpu.SemaphoreType.REGULAR,
        ]
        + [pltpu.VMEM(x.shape, x.dtype) for x in staged],
        compiler_params=pltpu.CompilerParams(
            collective_id=0, has_side_effects=True, vmem_limit_bytes=48 * 1024 * 1024
        ),
    )(patch_count, *[pltpu.with_memory_space_constraint(x, pltpu.HBM) for x in inputs])
    merged, anomaly = pl.pallas_call(
        store_kernel,
        out_shape=shapes,
        in_specs=[vmem] * 4,
        out_specs=(hbm, hbm),
        scratch_shapes=[
            pltpu.VMEM((chunks, nv, patches // chunks), F32),
            pltpu.SemaphoreType.DMA((chunks + 1,)),
        ],
        compiler_params=pltpu.CompilerParams(vmem_limit_bytes=8 * 1024 * 1024),
    )(*results)
    return merged.T, anomaly.T[None]


def solution(mesh):
    split = P(("clump", "grp"))
    return jax.shard_map(
        per_device,
        mesh=mesh,
        in_specs=(split,) * 10 + (P(),) + (split,) * 2,
        out_specs=(split, split),
        check_vma=False,
    )
```

```python
import functools

import jax
import jax.numpy as jnp
from jax import lax
from jax.experimental import pallas as pl
from jax.experimental.pallas import tpu as pltpu
from jax.sharding import PartitionSpec as P

MESH = pl.DeviceIdType.MESH
F32 = jnp.float32
BF16 = jnp.bfloat16
INPUTS = 12


def iota(shape, dim):
    return lax.broadcasted_iota(jnp.int32, shape, dim)


def onehot(mask):
    return jnp.where(mask, 1.0, 0.0).astype(BF16)


def halves(x):
    high = x.astype(BF16)
    return high, (x - high.astype(F32)).astype(BF16)


def dot(a, b):
    return jnp.dot(a, b, preferred_element_type=F32)


def dot_nt(a, b):
    return lax.dot_general(a, b, (((1,), (1,)), ((), ())), preferred_element_type=F32)


def rows_of(rows, total):
    n = rows[0].shape[1]
    at = iota((total, n), 0)
    out = jnp.zeros((total, n), F32)
    for k, row in enumerate(rows):
        out = jnp.where(at == k, jnp.broadcast_to(row.astype(F32), (total, n)), out)
    return out.astype(BF16)


def split_by(x, size):
    if size & (size - 1) == 0:
        return lax.shift_right_logical(x, jnp.int32(size.bit_length() - 1)), x & (size - 1)
    return x // size, x % size


def select(table, chosen):
    high, low = halves(table)
    both = dot(jnp.concatenate([high, low], axis=0), chosen)
    return both[: table.shape[0]] + both[table.shape[0] :]


def wide(one, two):
    blank = jnp.zeros(one.shape, BF16)

    def beside(first, second):
        upper = jnp.concatenate([first, blank], axis=1)
        return jnp.concatenate([upper, jnp.concatenate([blank, second], axis=1)], axis=0)

    (high, low), (high_two, low_two) = halves(one), halves(two)
    return beside(high, high_two), beside(low, low_two)


def pack_wide(chosen, parts):
    rows = chosen.shape[0] // 2
    pair = jnp.concatenate([chosen[:rows], chosen[rows:]], axis=1)
    return dot_nt(pair, parts[0]) + dot_nt(pair, parts[1])


def pack(chosen, x):
    return pack_wide(chosen, wide(x, x))


def unpack(packed):
    turned = packed.T
    middle = turned.shape[0] // 2
    return jnp.concatenate([turned[:middle], turned[middle:]], axis=1)


def kernel(
    n_clump, n_group, inner_clump, inner_group, cap, slots, half, stride,
    *refs,
):
    count_ref, *refs = refs
    sources, refs = refs[:INPUTS], refs[INPUTS:]
    merged_ref, base_ref, patch_of_ref, answers_ref = refs[:4]
    tables, own, ask, asked, note, noted, fore, reply, back, send, recv = refs[4:15]
    send_sem, recv_sem, in_sem, known = refs[15:19]
    staged = refs[19:]
    (
        target_ref, lwt_ref, lgrid_ref, clu_ref, cwt_ref, pcol_ref, pwt_ref,
        scale_ref, pft_ref, flux_ref,
    ) = staged
    nv, patches = flux_ref.shape
    types = scale_ref.shape[0]
    cols = cwt_ref.shape[1]
    lus = lwt_ref.shape[1]
    cells = target_ref.shape[1]
    n = n_clump * n_group
    rows = n * stride
    outer_clump, outer_group = n_clump // inner_clump, n_group // inner_group
    places, askers = inner_clump * outer_group, outer_clump * inner_group
    sharers = places * inner_group
    pairs = sharers // 2
    field_ref, frac_ref = own.at[pl.ds(0, nv)], own.at[pl.ds(nv, 1)]
    loads = [
        pltpu.make_async_copy(source, into, in_sem.at[0 if k == 0 else 2 if k < 10 else 1])
        for k, (source, into) in enumerate(zip(sources, (*staged, frac_ref, field_ref)))
    ]
    my_clump, my_group = lax.axis_index("clump"), lax.axis_index("grp")
    my_slab, my_row = lax.div(my_clump, inner_clump), lax.rem(my_clump, inner_clump)
    my_side, my_core = lax.div(my_group, inner_group), lax.rem(my_group, inner_group)
    keeper = inner_group - 1
    keeps = my_core == keeper

    def ahead_of(mine, step, size):
        there = mine + step
        return jnp.where(there >= size, there - size, there)

    def behind(mine, step, size):
        there = mine - step
        return jnp.where(there < 0, there + size, there)

    def offsets(act, outer, inner, own=False, far_first=False):
        if outer <= 8:
            steps = [(o, i) for o in range(outer) for i in range(inner) if own or o or i]
            for o, i in steps[::-1] if far_first else steps:
                act(o * inner + i, o, i)
        else:
            for i in range(0 if own else 1, inner):
                act(i, 0, i)

            @pl.loop(1, outer)
            def _(o):
                for i in range(inner):
                    act(o * inner + i, o, i)

    def place(there, row, side, slab, core):
        slab, row = there(my_slab, slab, outer_clump), there(my_row, row, inner_clump)
        side, core = there(my_side, side, outer_group), there(my_core, core, inner_group)
        return slab * inner_clump + row, side * inner_group + core

    def each_other(act, there):
        for row in range(inner_clump - 1, -1, -1):
            for side in range(outer_group - 1, -1, -1):
                t = row * outer_group + side

                def one(block, o, i, t=t, row=row, side=side):
                    act(t * askers + block, place(there, row, side, o, i))

                offsets(one, outer_clump, inner_group, own=t > 0)

    def remote(source, into, k, device):
        sent = 1 if k == 3 else 0
        pltpu.make_async_remote_copy(
            src_ref=source,
            dst_ref=into,
            send_sem=send_sem.at[sent],
            recv_sem=recv_sem.at[k],
            device_id=device,
            device_id_type=MESH,
        ).start()

    def wait(rest, sem):
        pltpu.make_async_copy(rest, rest, sem).wait()

    barrier = pltpu.get_barrier_semaphore()

    def signal(sem, device):
        pl.semaphore_signal(sem, inc=1, device_id=device, device_id_type=MESH)

    def each_place(act, there):
        def one(block, o, i):
            act(block, place(there, o, i, 0, 0))

        offsets(one, inner_clump, outer_group, far_first=True)

    def slabs(act):
        if outer_clump <= 8:
            for o in range(1, outer_clump):
                act(o)
        else:
            pl.loop(1, outer_clump)(act)

    def each_slab(act, there):
        slabs(lambda o: act(o, place(there, 0, 0, o, 0)))

    def core_of(device, core):
        return device[0], device[1] - my_core + core

    def keeper_of(device):
        return core_of(device, keeper)

    here = (my_clump, my_group)
    last_place = (my_row == inner_clump - 1) & (my_side == outer_group - 1)
    last_plane = my_slab == outer_clump - 1
    last_chip = last_place & last_plane
    last = last_chip & keeps

    def greet(step, device):
        for core in range(inner_group):
            signal(barrier, core_of(device, core))

    @pl.when(keeps)
    def _():
        each_slab(lambda o, device: signal(barrier, keeper_of(device)), ahead_of)
        each_place(greet, ahead_of)
        for core in range(keeper):
            signal(barrier, core_of(here, core))

    @pl.when(jnp.logical_not(keeps))
    def _():
        signal(barrier, keeper_of(here))

    @pl.when(jnp.logical_not(keeps & (last_place | last_plane) | last_chip))
    def _():
        signal(barrier, (n_clump - 1, n_group - 1))

    for k in (0, 10, 11, *range(1, 10)):
        loads[k].start()

    table_rows = pl.ds(0, nv + 1)

    def share(block, device):
        into = tables.at[block * inner_group + my_core, table_rows]
        remote(own.at[table_rows], into, 0, keeper_of(device))

    def enter():
        loads[10].wait()
        loads[11].wait()
        near = places - 1 + jnp.where(keeps, outer_clump - 1 + keeper, 1)
        pl.semaphore_wait(barrier, jnp.where(last, n - 1, near))
        each_place(share, ahead_of)

        @pl.when(keeps)
        def _():
            for core in range(keeper):
                signal(known.at[0], core_of(here, core))

        @pl.when(jnp.logical_not(keeps))
        def _():
            share(0, here)

        @pl.when(last)
        def _():
            each_other(lambda block, device: signal(known.at[1], device), ahead_of)

    pl.when(last_chip)(enter)
    loads[0].wait()
    target = target_ref[...]
    owner, local = split_by(target, cells)
    owner_b = jnp.broadcast_to(owner.astype(F32), (cells, cells))
    same = owner_b == owner_b.T
    earlier = iota((cells, cells), 0) < iota((cells, cells), 1)
    rank = jnp.sum(jnp.where(same & earlier, 1.0, 0.0), axis=0, keepdims=True).astype(jnp.int32)
    to_clump, to_group = split_by(owner, n_group)
    to_slab, to_row = split_by(to_clump, inner_clump)
    to_side, to_core = split_by(to_group, inner_group)
    table = behind(my_row, to_row, inner_clump) * outer_group
    table = table + behind(my_side, to_side, outer_group)
    entry = table * inner_group + to_core
    slab = behind(to_slab, my_slab, outer_clump)
    wanted = (local + 1).astype(F32)
    asks = jnp.where(iota((outer_clump, cells), 0) == slab, wanted, 0.0).astype(BF16)
    ask_rows = dot_nt(asks, onehot(iota((128, cells), 0) == entry * slots + rank))
    for k in range(outer_clump):
        ask[k, 0:1, :] = ask_rows[k : k + 1]
    one_row = pl.ds(0, 1)
    pl.when(jnp.logical_not(last_chip))(enter)

    def request(step, device):
        into = asked.at[step * inner_group + my_core, one_row]
        remote(ask.at[step, one_row], into, 1, keeper_of(device))

    @pl.when(jnp.logical_not(keeps))
    def _():
        request(0, here)

    @pl.when(jnp.logical_not(keeps))
    def _():
        pl.semaphore_wait(known.at[0], 1)

    each_slab(request, ahead_of)
    frac = frac_ref[...]
    block = behind(to_row, my_row, inner_clump) * outer_group
    block = (block + behind(to_side, my_side, outer_group)) * outer_clump + slab
    block = (block * inner_group + behind(to_core, my_core, inner_group)) * stride
    part, line = split_by(rank, half)
    slot_of = onehot(iota((2 * rows, cells), 0) == part * rows + block + line)
    asks = jnp.where(iota((rows, cells), 0) == block, wanted, 0.0).astype(BF16)
    id_rows = dot_nt(asks, onehot(iota((128, cells), 0) == rank))
    in_stride = split_by(iota((rows, 128), 0), stride)[1]
    note[...] = jnp.where(in_stride == 1, jnp.broadcast_to(frac, (rows, cells)), id_rows)
    noted[0:2, :] = note[0:2, :]

    def lines_of(block, count):
        start = block * stride
        return pl.ds(start if isinstance(start, int) else pl.multiple_of(start, stride), count)

    def give_note(block, device):
        its = lines_of(block, 2)
        remote(note.at[its], noted.at[its], 4, device)

    @pl.when(last_chip)
    def _():
        @pl.when(jnp.logical_not(last))
        def _():
            pl.semaphore_wait(known.at[1], 1)

        each_other(give_note, ahead_of)


    for load in loads[1:10]:
        load.wait()
    lu_hi, lu_lo = halves(lwt_ref[...])
    lu_rows = rows_of([lu_hi, lu_lo, lgrid_ref[...]], 16)
    lu_of = onehot(iota((lus, cols), 0) == clu_ref[...])
    col_vals = dot(lu_rows, lu_of)
    col_w = cwt_ref[...] * (col_vals[0:1] + col_vals[1:2])

    c_hi, c_lo = halves(col_w)
    col_rows = rows_of([c_hi, c_lo, col_vals[2:3]], 16)
    col_of = onehot(iota((cols, patches), 0) == pcol_ref[...])
    patch_vals = dot(col_rows, col_of)
    alive = jnp.where(iota((1, patches), 1) < count_ref[0], 1.0, 0.0)
    weight = alive * pwt_ref[...] * (patch_vals[0:1] + patch_vals[1:2])
    home = patch_vals[2:3].astype(jnp.int32)
    home_of = onehot(iota((cells, patches), 0) == home)

    scales = scale_ref[...]
    t1 = scales.astype(BF16).astype(F32)
    t2 = (scales - t1).astype(BF16).astype(F32)
    t3 = scales - t1 - t2
    pad = 128 - 3 * types
    stacked = jnp.concatenate([t1, t2, t3, jnp.zeros((pad, nv), F32)], axis=0)
    stacked = jnp.concatenate([stacked, jnp.zeros((128, 128 - nv), F32)], axis=1)
    scale_t = stacked.T[:nv].astype(BF16)
    kind = iota((128, patches), 0)
    type_of = onehot(
        (kind == pft_ref[...])
        | (kind == pft_ref[...] + types)
        | (kind == pft_ref[...] + 2 * types)
    )
    scaled = flux_ref[...] * dot(scale_t, type_of)

    x_hi, x_lo = halves(scaled * weight)
    w_hi, w_lo = halves(weight)
    sums = dot_nt(
        jnp.concatenate([x_hi, x_lo, rows_of([w_hi, w_lo], 16)], axis=0), home_of
    )
    num = sums[:nv] + sums[nv : 2 * nv]
    den = sums[2 * nv : 2 * nv + 1] + sums[2 * nv + 1 : 2 * nv + 2]
    mean = num / jnp.maximum(den, 1.0)

    send[...] = pack(slot_of, mean)
    recv[0:half, :] = send[0:half, :]
    @pl.when(jnp.logical_not(last_chip))
    def _():
        pl.semaphore_wait(known.at[1], 1)
        each_other(give_note, ahead_of)

    def give(block, device):
        its = lines_of(block, half)
        remote(send.at[its], recv.at[its], 2, device)

    each_other(give, ahead_of)

    @pl.when(keeps)
    def _():
        asked[keeper, 0:1, :] = ask[0, 0:1, :]
        wait(asked.at[pl.ds(0, askers - 1), one_row], recv_sem.at[1])

        def picks(told, count):
            height = count * slots
            told = jnp.broadcast_to(told, (count, slots, 128)).reshape(height, 128)
            lane_less = iota((height, 128), 1) - split_by(iota((height, 128), 0), slots)[1]
            spread = [jnp.where(lane_less == t * slots, told, 0.0) for t in range(sharers)]
            ids = dot(jnp.concatenate(spread, axis=0).astype(BF16), jnp.ones((128, cells), BF16))
            return onehot(ids == (iota(ids.shape, 1) + 1).astype(F32))

        def fill(into, chosen, count):
            for p in range(pairs):
                one, end = 2 * p * count * slots, 2 * (p + 1) * count * slots
                packed = pack_wide(chosen[one:end], held[p])
                into[:, p * slots : (p + 1) * slots, :] = packed.reshape(count, slots, 128)

        first = pl.ds(my_slab * inner_group, inner_group)
        first_picks = picks(asked[first, 0:1, :], inner_group)
        wait(tables.at[pl.ds(0, sharers - 1), table_rows], recv_sem.at[0])
        held = [own if t == keeper else tables.at[t] for t in range(sharers)]
        held = [(1.0 - x[nv : nv + 1, :]) * x[0:nv, :] for x in held]
        held = [wide(held[2 * p], held[2 * p + 1]) for p in range(pairs)]
        fill(fore, first_picks, inner_group)
        for i in range(inner_group):

            @pl.when((my_slab > 0) | (i < keeper))
            def _(i=i):
                remote(fore.at[i], back.at[my_slab], 3, (my_row, my_group - my_core + i))

        fill(reply, picks(asked[:, 0:1, :], askers), askers)

        def respond(o):
            clump, group = place(behind, 0, 0, o, 0)
            for i in range(keeper if isinstance(o, int) and o == 0 else inner_group):
                source = reply.at[o * inner_group + i]
                remote(source, back.at[o], 3, (clump, group - my_core + i))

        def respond_rest(o):
            pl.when(my_slab != o)(lambda: respond(o))

        respond_rest(0)
        slabs(respond_rest)
        back[0] = reply[keeper]

    other = (1.0 - frac) * field_ref[...]
    pair, side = split_by(entry, 2)
    answers = outer_clump * pairs * slots
    spot = side * answers + (slab * pairs + pair) * slots + rank
    answer_of = onehot(iota((2 * answers, cells), 0) == spot)
    patch_of_ref[...] = (dot(answer_of, home_of) * alive).astype(BF16)

    flat = pl.ds(0, (n - 1) * half)
    keeps_or_not = ((keeps, 1), (jnp.logical_not(keeps), 0))
    for which, first in keeps_or_not:

        @pl.when(which)
        def _(first=first):
            wait(tables.at[pl.ds(0, places - first), table_rows], send_sem.at[0])
            wait(ask.at[pl.ds(0, outer_clump - first), one_row], send_sem.at[0])

    wait(send.at[flat], send_sem.at[0])
    wait(note.at[pl.ds(0, (n - 1) * 2)], send_sem.at[0])
    wait(noted.at[pl.ds(0, (n - 1) * 2)], recv_sem.at[4])
    lane = iota((2 * rows, 128), 0)
    lane_part = jnp.where(lane >= rows, 1, 0)
    lane_line = split_by(lane - lane_part * rows, stride)[1]
    its_lane = (lane_line < half) & (
        iota((2 * rows, 128), 1) == lane_part * half + lane_line
    )
    told = jnp.where(in_stride < 2, noted[...], 0.0)
    ids_of = jnp.broadcast_to(told.reshape(n, stride, 128)[:, 0:1, :], (n, stride, 128)).reshape(rows, 128)
    spread = jnp.where(its_lane, jnp.concatenate([ids_of, ids_of], axis=0), 0.0).astype(BF16)
    ids = dot(spread, jnp.ones((128, cells), BF16))
    owned_of = onehot(ids == (iota((2 * rows, cells), 1) + 1).astype(F32))

    back_of = (table * outer_clump + behind(my_slab, to_slab, outer_clump)) * inner_group
    back_of = (back_of + behind(my_core, to_core, inner_group)) * stride + 1
    all_frac = select(told.T, onehot(iota((rows, cells), 0) == back_of))
    cell_frac = jnp.sum(
        jnp.where(iota((128, cells), 0) == local, all_frac, 0.0), axis=0, keepdims=True
    )
    base_ref[...] = alive * (scaled - select(cell_frac * mean, home_of))

    @pl.when(keeps)
    def _():
        wait(reply.at[pl.ds(0, askers - 1)], send_sem.at[1])

    wait(recv.at[flat], recv_sem.at[2])
    in_half = split_by(iota((rows, 128), 0), stride)[1] < half
    owned = select(unpack(jnp.where(in_half, recv[...], 0.0)), owned_of)
    merged_ref[...] = frac * owned + other

    for which, first in keeps_or_not:

        @pl.when(which)
        def _(first=first):
            wait(back.at[pl.ds(first, outer_clump - first)], recv_sem.at[3])

    answers_ref[...] = back[...].reshape(answers, 128)


def store_kernel(merged, base, patch_of, answers, merged_out, anomaly_out, anomaly, sem):
    chunks = anomaly.shape[0]
    width = anomaly.shape[2]
    stores = [pltpu.make_async_copy(merged, merged_out, sem.at[chunks])]
    stores[0].start()
    high, low = halves(unpack(answers[...]))
    table = jnp.concatenate([high, low], axis=0)
    for k in range(chunks):
        its = pl.ds(k * width, width)
        both = dot(table, patch_of[:, its])
        anomaly[k] = base[:, its] - (both[: high.shape[0]] + both[high.shape[0] :])
        stores.append(pltpu.make_async_copy(anomaly.at[k], anomaly_out.at[:, its], sem.at[k]))
        stores[-1].start()
    for store in stores:
        store.wait()


def per_device(
    flux, patch_pft, patch_wt, patch_col, col_wt, col_lu, lu_wt, lu_grid, cell_target,
    patch_count, pft_scale, cpl_frac, cpl_field,
):
    n_clump = lax.axis_size("clump")
    n_group = lax.axis_size("grp")
    n = n_clump * n_group
    nv = flux.shape[2]
    patches = flux.shape[1]
    cells = cell_target.shape[1]
    inner_group = 2 if n_group % 2 == 0 else 1
    outer_group = n_group // inner_group
    inner_clump = outer_group if n_clump % outer_group == 0 else 1
    sharers = inner_clump * n_group
    outer_clump = n_clump // inner_clump
    askers = outer_clump * inner_group
    cap = max(2, 2 * cells // n)
    half = -(-cap // 2)
    slots = -(-cap // 8) * 8
    stride = -(-half // 8) * 8
    answers = outer_clump * (sharers // 2) * slots
    chunks = 2
    vmem = pl.BlockSpec(memory_space=pltpu.VMEM)
    hbm = pl.BlockSpec(memory_space=pltpu.HBM)
    staged = (
        cell_target, lu_wt, lu_grid, col_lu, col_wt, patch_col, patch_wt,
        pft_scale, patch_pft, flux[0].T,
    )
    inputs = (*staged, cpl_frac.reshape(1, -1), cpl_field.T)
    shapes = (
        jax.ShapeDtypeStruct((nv, cells), F32),
        jax.ShapeDtypeStruct((nv, patches), F32),
    )
    results = pl.pallas_call(
        functools.partial(
            kernel, n_clump, n_group, inner_clump, inner_group, cap, slots, half, stride
        ),
        out_shape=(
            pltpu.VMEM((nv, cells), F32),
            pltpu.VMEM((nv, patches), F32),
            pltpu.VMEM((2 * answers, patches), BF16),
            pltpu.VMEM((answers, 128), F32),
        ),
        in_specs=[pl.BlockSpec(memory_space=pltpu.SMEM)] + [hbm] * INPUTS,
        out_specs=(vmem,) * 4,
        scratch_shapes=[
            pltpu.VMEM((sharers, -(-(nv + 1) // 8) * 8, cells), F32),
            pltpu.VMEM((-(-(nv + 1) // 8) * 8, cells), F32),
            pltpu.VMEM((outer_clump, 8, 128), F32),
            pltpu.VMEM((askers, 8, 128), F32),
            pltpu.VMEM((n * stride, 128), F32),
            pltpu.VMEM((n * stride, 128), F32),
            pltpu.VMEM((inner_group, sharers // 2 * slots, 128), F32),
            pltpu.VMEM((askers, sharers // 2 * slots, 128), F32),
            pltpu.VMEM((outer_clump, sharers // 2 * slots, 128), F32),
            pltpu.VMEM((n * stride, 128), F32),
            pltpu.VMEM((n * stride, 128), F32),
            pltpu.SemaphoreType.DMA((2,)),
            pltpu.SemaphoreType.DMA((5,)),
            pltpu.SemaphoreType.DMA((3,)),
            pltpu.SemaphoreType.REGULAR((2,)),
        ]
        + [pltpu.VMEM(x.shape, x.dtype) for x in staged],
        compiler_params=pltpu.CompilerParams(
            collective_id=0, has_side_effects=True, vmem_limit_bytes=48 * 1024 * 1024
        ),
    )(patch_count, *[pltpu.with_memory_space_constraint(x, pltpu.HBM) for x in inputs])
    merged, anomaly = pl.pallas_call(
        store_kernel,
        out_shape=shapes,
        in_specs=[vmem] * 4,
        out_specs=(hbm, hbm),
        scratch_shapes=[
            pltpu.VMEM((chunks, nv, patches // chunks), F32),
            pltpu.SemaphoreType.DMA((chunks + 1,)),
        ],
        compiler_params=pltpu.CompilerParams(vmem_limit_bytes=8 * 1024 * 1024),
    )(*results)
    return merged.T, anomaly.T[None]


def solution(mesh):
    split = P(("clump", "grp"))
    return jax.shard_map(
        per_device,
        mesh=mesh,
        in_specs=(split,) * 10 + (P(),) + (split,) * 2,
        out_specs=(split, split),
        check_vma=False,
    )
```

```python
import functools

import jax
import jax.numpy as jnp
from jax import lax
from jax.experimental import pallas as pl
from jax.experimental.pallas import tpu as pltpu
from jax.sharding import PartitionSpec as P

MESH = pl.DeviceIdType.MESH
F32 = jnp.float32
BF16 = jnp.bfloat16
INPUTS = 12


def iota(shape, dim):
    return lax.broadcasted_iota(jnp.int32, shape, dim)


def onehot(mask):
    return jnp.where(mask, 1.0, 0.0).astype(BF16)


def halves(x):
    high = x.astype(BF16)
    return high, (x - high.astype(F32)).astype(BF16)


def dot(a, b):
    return jnp.dot(a, b, preferred_element_type=F32)


def dot_nt(a, b):
    return lax.dot_general(a, b, (((1,), (1,)), ((), ())), preferred_element_type=F32)


def rows_of(rows, total):
    n = rows[0].shape[1]
    at = iota((total, n), 0)
    out = jnp.zeros((total, n), F32)
    for k, row in enumerate(rows):
        out = jnp.where(at == k, jnp.broadcast_to(row.astype(F32), (total, n)), out)
    return out.astype(BF16)


def split_by(x, size):
    if size & (size - 1) == 0:
        return lax.shift_right_logical(x, jnp.int32(size.bit_length() - 1)), x & (size - 1)
    return x // size, x % size


def select(table, chosen):
    high, low = halves(table)
    both = dot(jnp.concatenate([high, low], axis=0), chosen)
    return both[: table.shape[0]] + both[table.shape[0] :]


def wide(one, two):
    blank = jnp.zeros(one.shape, BF16)

    def beside(first, second):
        upper = jnp.concatenate([first, blank], axis=1)
        return jnp.concatenate([upper, jnp.concatenate([blank, second], axis=1)], axis=0)

    (high, low), (high_two, low_two) = halves(one), halves(two)
    return beside(high, high_two), beside(low, low_two)


def pack_wide(chosen, parts):
    rows = chosen.shape[0] // 2
    pair = jnp.concatenate([chosen[:rows], chosen[rows:]], axis=1)
    return dot_nt(pair, parts[0]) + dot_nt(pair, parts[1])


def pack(chosen, x):
    return pack_wide(chosen, wide(x, x))


def unpack(packed):
    turned = packed.T
    middle = turned.shape[0] // 2
    return jnp.concatenate([turned[:middle], turned[middle:]], axis=1)


def kernel(
    n_clump, n_group, inner_clump, inner_group, cap, slots, half, stride,
    *refs,
):
    count_ref, *refs = refs
    sources, refs = refs[:INPUTS], refs[INPUTS:]
    got_ref, owned_of_ref, frac_out, other_ref, base_ref, patch_of_ref, answers_ref = refs[:7]
    tables, own, ask, asked, note, noted, fore, reply, back, send, recv = refs[7:18]
    send_sem, recv_sem, in_sem, known = refs[18:22]
    staged = refs[22:]
    (
        target_ref, lwt_ref, lgrid_ref, clu_ref, cwt_ref, pcol_ref, pwt_ref,
        scale_ref, pft_ref, flux_ref,
    ) = staged
    nv, patches = flux_ref.shape
    types = scale_ref.shape[0]
    cols = cwt_ref.shape[1]
    lus = lwt_ref.shape[1]
    cells = target_ref.shape[1]
    n = n_clump * n_group
    rows = n * stride
    outer_clump, outer_group = n_clump // inner_clump, n_group // inner_group
    places, askers = inner_clump * outer_group, outer_clump * inner_group
    sharers = places * inner_group
    pairs = sharers // 2
    field_ref, frac_ref = own.at[pl.ds(0, nv)], own.at[pl.ds(nv, 1)]
    loads = [
        pltpu.make_async_copy(source, into, in_sem.at[0 if k == 0 else 2 if k < 10 else 1])
        for k, (source, into) in enumerate(zip(sources, (*staged, frac_ref, field_ref)))
    ]
    my_clump, my_group = lax.axis_index("clump"), lax.axis_index("grp")
    my_slab, my_row = lax.div(my_clump, inner_clump), lax.rem(my_clump, inner_clump)
    my_side, my_core = lax.div(my_group, inner_group), lax.rem(my_group, inner_group)
    keeper = inner_group - 1
    keeps = my_core == keeper

    def ahead_of(mine, step, size):
        there = mine + step
        return jnp.where(there >= size, there - size, there)

    def behind(mine, step, size):
        there = mine - step
        return jnp.where(there < 0, there + size, there)

    def offsets(act, outer, inner, own=False, far_first=False):
        if outer <= 8:
            steps = [(o, i) for o in range(outer) for i in range(inner) if own or o or i]
            for o, i in steps[::-1] if far_first else steps:
                act(o * inner + i, o, i)
        else:
            for i in range(0 if own else 1, inner):
                act(i, 0, i)

            @pl.loop(1, outer)
            def _(o):
                for i in range(inner):
                    act(o * inner + i, o, i)

    def place(there, row, side, slab, core):
        slab, row = there(my_slab, slab, outer_clump), there(my_row, row, inner_clump)
        side, core = there(my_side, side, outer_group), there(my_core, core, inner_group)
        return slab * inner_clump + row, side * inner_group + core

    def each_other(act, there):
        for row in range(inner_clump - 1, -1, -1):
            for side in range(outer_group - 1, -1, -1):
                t = row * outer_group + side

                def one(block, o, i, t=t, row=row, side=side):
                    act(t * askers + block, place(there, row, side, o, i))

                offsets(one, outer_clump, inner_group, own=t > 0)

    def remote(source, into, k, device):
        sent = 1 if k == 3 else 0
        pltpu.make_async_remote_copy(
            src_ref=source,
            dst_ref=into,
            send_sem=send_sem.at[sent],
            recv_sem=recv_sem.at[k],
            device_id=device,
            device_id_type=MESH,
        ).start()

    def wait(rest, sem):
        pltpu.make_async_copy(rest, rest, sem).wait()

    barrier = pltpu.get_barrier_semaphore()

    def signal(sem, device):
        pl.semaphore_signal(sem, inc=1, device_id=device, device_id_type=MESH)

    def each_place(act, there):
        def one(block, o, i):
            act(block, place(there, o, i, 0, 0))

        offsets(one, inner_clump, outer_group, far_first=True)

    def slabs(act):
        if outer_clump <= 8:
            for o in range(1, outer_clump):
                act(o)
        else:
            pl.loop(1, outer_clump)(act)

    def each_slab(act, there):
        slabs(lambda o: act(o, place(there, 0, 0, o, 0)))

    def core_of(device, core):
        return device[0], device[1] - my_core + core

    def keeper_of(device):
        return core_of(device, keeper)

    here = (my_clump, my_group)
    last_place = (my_row == inner_clump - 1) & (my_side == outer_group - 1)
    last_plane = my_slab == outer_clump - 1
    last_chip = last_place & last_plane
    last = last_chip & keeps

    def greet(step, device):
        for core in range(inner_group):
            signal(barrier, core_of(device, core))

    @pl.when(keeps)
    def _():
        each_slab(lambda o, device: signal(barrier, keeper_of(device)), ahead_of)
        each_place(greet, ahead_of)
        for core in range(keeper):
            signal(barrier, core_of(here, core))

    @pl.when(jnp.logical_not(keeps))
    def _():
        signal(barrier, keeper_of(here))

    @pl.when(jnp.logical_not(keeps & (last_place | last_plane) | last_chip))
    def _():
        signal(barrier, (n_clump - 1, n_group - 1))

    for k in (0, 10, 11, *range(1, 10)):
        loads[k].start()

    table_rows = pl.ds(0, nv + 1)

    def share(block, device):
        into = tables.at[block * inner_group + my_core, table_rows]
        remote(own.at[table_rows], into, 0, keeper_of(device))

    def enter():
        loads[10].wait()
        loads[11].wait()
        near = places - 1 + jnp.where(keeps, outer_clump - 1 + keeper, 1)
        pl.semaphore_wait(barrier, jnp.where(last, n - 1, near))
        each_place(share, ahead_of)

        @pl.when(keeps)
        def _():
            for core in range(keeper):
                signal(known.at[0], core_of(here, core))

        @pl.when(jnp.logical_not(keeps))
        def _():
            share(0, here)

        @pl.when(last)
        def _():
            each_other(lambda block, device: signal(known.at[1], device), ahead_of)

    pl.when(last_chip)(enter)
    loads[0].wait()
    target = target_ref[...]
    owner, local = split_by(target, cells)
    owner_b = jnp.broadcast_to(owner.astype(F32), (cells, cells))
    same = owner_b == owner_b.T
    earlier = iota((cells, cells), 0) < iota((cells, cells), 1)
    rank = jnp.sum(jnp.where(same & earlier, 1.0, 0.0), axis=0, keepdims=True).astype(jnp.int32)
    to_clump, to_group = split_by(owner, n_group)
    to_slab, to_row = split_by(to_clump, inner_clump)
    to_side, to_core = split_by(to_group, inner_group)
    table = behind(my_row, to_row, inner_clump) * outer_group
    table = table + behind(my_side, to_side, outer_group)
    entry = table * inner_group + to_core
    slab = behind(to_slab, my_slab, outer_clump)
    wanted = (local + 1).astype(F32)
    asks = jnp.where(iota((outer_clump, cells), 0) == slab, wanted, 0.0).astype(BF16)
    ask_rows = dot_nt(asks, onehot(iota((128, cells), 0) == entry * slots + rank))
    for k in range(outer_clump):
        ask[k, 0:1, :] = ask_rows[k : k + 1]
    one_row = pl.ds(0, 1)
    pl.when(jnp.logical_not(last_chip))(enter)

    def request(step, device):
        into = asked.at[step * inner_group + my_core, one_row]
        remote(ask.at[step, one_row], into, 1, keeper_of(device))

    @pl.when(jnp.logical_not(keeps))
    def _():
        request(0, here)

    @pl.when(jnp.logical_not(keeps))
    def _():
        pl.semaphore_wait(known.at[0], 1)

    each_slab(request, ahead_of)
    frac = frac_ref[...]
    block = behind(to_row, my_row, inner_clump) * outer_group
    block = (block + behind(to_side, my_side, outer_group)) * outer_clump + slab
    block = (block * inner_group + behind(to_core, my_core, inner_group)) * stride
    part, line = split_by(rank, half)
    slot_of = onehot(iota((2 * rows, cells), 0) == part * rows + block + line)
    asks = jnp.where(iota((rows, cells), 0) == block, wanted, 0.0).astype(BF16)
    id_rows = dot_nt(asks, onehot(iota((128, cells), 0) == rank))
    in_stride = split_by(iota((rows, 128), 0), stride)[1]
    note[...] = jnp.where(in_stride == 1, jnp.broadcast_to(frac, (rows, cells)), id_rows)
    noted[0:2, :] = note[0:2, :]

    def lines_of(block, count):
        start = block * stride
        return pl.ds(start if isinstance(start, int) else pl.multiple_of(start, stride), count)

    def give_note(block, device):
        its = lines_of(block, 2)
        remote(note.at[its], noted.at[its], 4, device)

    @pl.when(last_chip)
    def _():
        @pl.when(jnp.logical_not(last))
        def _():
            pl.semaphore_wait(known.at[1], 1)

        each_other(give_note, ahead_of)


    for load in loads[1:10]:
        load.wait()
    lu_hi, lu_lo = halves(lwt_ref[...])
    lu_rows = rows_of([lu_hi, lu_lo, lgrid_ref[...]], 16)
    lu_of = onehot(iota((lus, cols), 0) == clu_ref[...])
    col_vals = dot(lu_rows, lu_of)
    col_w = cwt_ref[...] * (col_vals[0:1] + col_vals[1:2])

    c_hi, c_lo = halves(col_w)
    col_rows = rows_of([c_hi, c_lo, col_vals[2:3]], 16)
    col_of = onehot(iota((cols, patches), 0) == pcol_ref[...])
    patch_vals = dot(col_rows, col_of)
    alive = jnp.where(iota((1, patches), 1) < count_ref[0], 1.0, 0.0)
    weight = alive * pwt_ref[...] * (patch_vals[0:1] + patch_vals[1:2])
    home = patch_vals[2:3].astype(jnp.int32)
    home_of = onehot(iota((cells, patches), 0) == home)

    scales = scale_ref[...]
    t1 = scales.astype(BF16).astype(F32)
    t2 = (scales - t1).astype(BF16).astype(F32)
    t3 = scales - t1 - t2
    pad = 128 - 3 * types
    stacked = jnp.concatenate([t1, t2, t3, jnp.zeros((pad, nv), F32)], axis=0)
    stacked = jnp.concatenate([stacked, jnp.zeros((128, 128 - nv), F32)], axis=1)
    scale_t = stacked.T[:nv].astype(BF16)
    kind = iota((128, patches), 0)
    type_of = onehot(
        (kind == pft_ref[...])
        | (kind == pft_ref[...] + types)
        | (kind == pft_ref[...] + 2 * types)
    )
    scaled = flux_ref[...] * dot(scale_t, type_of)

    x_hi, x_lo = halves(scaled * weight)
    w_hi, w_lo = halves(weight)
    sums = dot_nt(
        jnp.concatenate([x_hi, x_lo, rows_of([w_hi, w_lo], 16)], axis=0), home_of
    )
    num = sums[:nv] + sums[nv : 2 * nv]
    den = sums[2 * nv : 2 * nv + 1] + sums[2 * nv + 1 : 2 * nv + 2]
    mean = num / jnp.maximum(den, 1.0)

    send[...] = pack(slot_of, mean)
    recv[0:half, :] = send[0:half, :]
    @pl.when(jnp.logical_not(last_chip))
    def _():
        pl.semaphore_wait(known.at[1], 1)
        each_other(give_note, ahead_of)

    def give(block, device):
        its = lines_of(block, half)
        remote(send.at[its], recv.at[its], 2, device)

    each_other(give, ahead_of)

    @pl.when(keeps)
    def _():
        asked[keeper, 0:1, :] = ask[0, 0:1, :]
        wait(asked.at[pl.ds(0, askers - 1), one_row], recv_sem.at[1])

        def picks(told, count):
            height = count * slots
            told = jnp.broadcast_to(told, (count, slots, 128)).reshape(height, 128)
            lane_less = iota((height, 128), 1) - split_by(iota((height, 128), 0), slots)[1]
            spread = [jnp.where(lane_less == t * slots, told, 0.0) for t in range(sharers)]
            ids = dot(jnp.concatenate(spread, axis=0).astype(BF16), jnp.ones((128, cells), BF16))
            return onehot(ids == (iota(ids.shape, 1) + 1).astype(F32))

        def fill(into, chosen, count):
            for p in range(pairs):
                one, end = 2 * p * count * slots, 2 * (p + 1) * count * slots
                packed = pack_wide(chosen[one:end], held[p])
                into[:, p * slots : (p + 1) * slots, :] = packed.reshape(count, slots, 128)

        first = pl.ds(my_slab * inner_group, inner_group)
        first_picks = picks(asked[first, 0:1, :], inner_group)
        wait(tables.at[pl.ds(0, sharers - 1), table_rows], recv_sem.at[0])
        held = [own if t == keeper else tables.at[t] for t in range(sharers)]
        held = [(1.0 - x[nv : nv + 1, :]) * x[0:nv, :] for x in held]
        held = [wide(held[2 * p], held[2 * p + 1]) for p in range(pairs)]
        fill(fore, first_picks, inner_group)
        for i in range(inner_group):

            @pl.when((my_slab > 0) | (i < keeper))
            def _(i=i):
                remote(fore.at[i], back.at[my_slab], 3, (my_row, my_group - my_core + i))

        fill(reply, picks(asked[:, 0:1, :], askers), askers)

        def respond(o):
            clump, group = place(behind, 0, 0, o, 0)
            for i in range(keeper if isinstance(o, int) and o == 0 else inner_group):
                source = reply.at[o * inner_group + i]
                remote(source, back.at[o], 3, (clump, group - my_core + i))

        def respond_rest(o):
            pl.when(my_slab != o)(lambda: respond(o))

        respond_rest(0)
        slabs(respond_rest)
        back[0] = reply[keeper]

    other_ref[...] = (1.0 - frac) * field_ref[...]
    frac_out[...] = frac
    pair, side = split_by(entry, 2)
    answers = outer_clump * pairs * slots
    spot = side * answers + (slab * pairs + pair) * slots + rank
    answer_of = onehot(iota((2 * answers, cells), 0) == spot)
    patch_of_ref[...] = (dot(answer_of, home_of) * alive).astype(BF16)

    flat = pl.ds(0, (n - 1) * half)
    keeps_or_not = ((keeps, 1), (jnp.logical_not(keeps), 0))
    for which, first in keeps_or_not:

        @pl.when(which)
        def _(first=first):
            wait(tables.at[pl.ds(0, places - first), table_rows], send_sem.at[0])
            wait(ask.at[pl.ds(0, outer_clump - first), one_row], send_sem.at[0])

    wait(send.at[flat], send_sem.at[0])
    wait(note.at[pl.ds(0, (n - 1) * 2)], send_sem.at[0])
    wait(noted.at[pl.ds(0, (n - 1) * 2)], recv_sem.at[4])
    lane = iota((2 * rows, 128), 0)
    lane_part = jnp.where(lane >= rows, 1, 0)
    lane_line = split_by(lane - lane_part * rows, stride)[1]
    its_lane = (lane_line < half) & (
        iota((2 * rows, 128), 1) == lane_part * half + lane_line
    )
    told = jnp.where(in_stride < 2, noted[...], 0.0)
    ids_of = jnp.broadcast_to(told.reshape(n, stride, 128)[:, 0:1, :], (n, stride, 128)).reshape(rows, 128)
    spread = jnp.where(its_lane, jnp.concatenate([ids_of, ids_of], axis=0), 0.0).astype(BF16)
    ids = dot(spread, jnp.ones((128, cells), BF16))
    owned_of_ref[...] = onehot(ids == (iota((2 * rows, cells), 1) + 1).astype(F32))

    back_of = (table * outer_clump + behind(my_slab, to_slab, outer_clump)) * inner_group
    back_of = (back_of + behind(my_core, to_core, inner_group)) * stride + 1
    all_frac = select(told.T, onehot(iota((rows, cells), 0) == back_of))
    cell_frac = jnp.sum(
        jnp.where(iota((128, cells), 0) == local, all_frac, 0.0), axis=0, keepdims=True
    )
    base_ref[...] = alive * (scaled - select(cell_frac * mean, home_of))

    @pl.when(keeps)
    def _():
        wait(reply.at[pl.ds(0, askers - 1)], send_sem.at[1])

    for which, first in keeps_or_not:

        @pl.when(which)
        def _(first=first):
            wait(back.at[pl.ds(first, outer_clump - first)], recv_sem.at[3])

    wait(recv.at[flat], recv_sem.at[2])
    in_half = split_by(iota((rows, 128), 0), stride)[1] < half
    got_ref[...] = jnp.where(in_half, recv[...], 0.0)
    answers_ref[...] = back[...].reshape(answers, 128)


def store_kernel(
    got, owned_of, frac, other, base, patch_of, answers,
    merged_out, anomaly_out, merged, anomaly, sem,
):
    chunks = anomaly.shape[0]
    width = anomaly.shape[2]
    stores = []
    high, low = halves(unpack(answers[...]))
    table = jnp.concatenate([high, low], axis=0)
    for k in range(chunks):
        its = pl.ds(k * width, width)
        both = dot(table, patch_of[:, its])
        anomaly[k] = base[:, its] - (both[: high.shape[0]] + both[high.shape[0] :])
        stores.append(pltpu.make_async_copy(anomaly.at[k], anomaly_out.at[:, its], sem.at[k]))
        stores[-1].start()
    merged[...] = frac[...] * select(unpack(got[...]), owned_of[...]) + other[...]
    stores.append(pltpu.make_async_copy(merged, merged_out, sem.at[chunks]))
    stores[-1].start()
    for store in stores:
        store.wait()


def per_device(
    flux, patch_pft, patch_wt, patch_col, col_wt, col_lu, lu_wt, lu_grid, cell_target,
    patch_count, pft_scale, cpl_frac, cpl_field,
):
    n_clump = lax.axis_size("clump")
    n_group = lax.axis_size("grp")
    n = n_clump * n_group
    nv = flux.shape[2]
    patches = flux.shape[1]
    cells = cell_target.shape[1]
    inner_group = 2 if n_group % 2 == 0 else 1
    outer_group = n_group // inner_group
    inner_clump = outer_group if n_clump % outer_group == 0 else 1
    sharers = inner_clump * n_group
    outer_clump = n_clump // inner_clump
    askers = outer_clump * inner_group
    cap = max(2, 2 * cells // n)
    half = -(-cap // 2)
    slots = -(-cap // 8) * 8
    stride = -(-half // 8) * 8
    answers = outer_clump * (sharers // 2) * slots
    chunks = 2
    vmem = pl.BlockSpec(memory_space=pltpu.VMEM)
    hbm = pl.BlockSpec(memory_space=pltpu.HBM)
    staged = (
        cell_target, lu_wt, lu_grid, col_lu, col_wt, patch_col, patch_wt,
        pft_scale, patch_pft, flux[0].T,
    )
    inputs = (*staged, cpl_frac.reshape(1, -1), cpl_field.T)
    shapes = (
        jax.ShapeDtypeStruct((nv, cells), F32),
        jax.ShapeDtypeStruct((nv, patches), F32),
    )
    results = pl.pallas_call(
        functools.partial(
            kernel, n_clump, n_group, inner_clump, inner_group, cap, slots, half, stride
        ),
        out_shape=(
            pltpu.VMEM((n * stride, 128), F32),
            pltpu.VMEM((2 * n * stride, cells), BF16),
            pltpu.VMEM((1, cells), F32),
            pltpu.VMEM((nv, cells), F32),
            pltpu.VMEM((nv, patches), F32),
            pltpu.VMEM((2 * answers, patches), BF16),
            pltpu.VMEM((answers, 128), F32),
        ),
        in_specs=[pl.BlockSpec(memory_space=pltpu.SMEM)] + [hbm] * INPUTS,
        out_specs=(vmem,) * 7,
        scratch_shapes=[
            pltpu.VMEM((sharers, -(-(nv + 1) // 8) * 8, cells), F32),
            pltpu.VMEM((-(-(nv + 1) // 8) * 8, cells), F32),
            pltpu.VMEM((outer_clump, 8, 128), F32),
            pltpu.VMEM((askers, 8, 128), F32),
            pltpu.VMEM((n * stride, 128), F32),
            pltpu.VMEM((n * stride, 128), F32),
            pltpu.VMEM((inner_group, sharers // 2 * slots, 128), F32),
            pltpu.VMEM((askers, sharers // 2 * slots, 128), F32),
            pltpu.VMEM((outer_clump, sharers // 2 * slots, 128), F32),
            pltpu.VMEM((n * stride, 128), F32),
            pltpu.VMEM((n * stride, 128), F32),
            pltpu.SemaphoreType.DMA((2,)),
            pltpu.SemaphoreType.DMA((5,)),
            pltpu.SemaphoreType.DMA((3,)),
            pltpu.SemaphoreType.REGULAR((2,)),
        ]
        + [pltpu.VMEM(x.shape, x.dtype) for x in staged],
        compiler_params=pltpu.CompilerParams(
            collective_id=0, has_side_effects=True, vmem_limit_bytes=48 * 1024 * 1024
        ),
    )(patch_count, *[pltpu.with_memory_space_constraint(x, pltpu.HBM) for x in inputs])
    merged, anomaly = pl.pallas_call(
        store_kernel,
        out_shape=shapes,
        in_specs=[vmem] * 7,
        out_specs=(hbm, hbm),
        scratch_shapes=[
            pltpu.VMEM((nv, cells), F32),
            pltpu.VMEM((chunks, nv, patches // chunks), F32),
            pltpu.SemaphoreType.DMA((chunks + 1,)),
        ],
        compiler_params=pltpu.CompilerParams(vmem_limit_bytes=8 * 1024 * 1024),
    )(*results)
    return merged.T, anomaly.T[None]


def solution(mesh):
    split = P(("clump", "grp"))
    return jax.shard_map(
        per_device,
        mesh=mesh,
        in_specs=(split,) * 10 + (P(),) + (split,) * 2,
        out_specs=(split, split),
        check_vma=False,
    )
```

```python
import functools

import jax
import jax.numpy as jnp
from jax import lax
from jax.experimental import pallas as pl
from jax.experimental.pallas import tpu as pltpu
from jax.sharding import PartitionSpec as P

MESH = pl.DeviceIdType.MESH
F32 = jnp.float32
BF16 = jnp.bfloat16
INPUTS = 12


def iota(shape, dim):
    return lax.broadcasted_iota(jnp.int32, shape, dim)


def onehot(mask):
    return jnp.where(mask, 1.0, 0.0).astype(BF16)


def halves(x):
    high = x.astype(BF16)
    return high, (x - high.astype(F32)).astype(BF16)


def dot(a, b):
    return jnp.dot(a, b, preferred_element_type=F32)


def dot_nt(a, b):
    return lax.dot_general(a, b, (((1,), (1,)), ((), ())), preferred_element_type=F32)


def rows_of(rows, total):
    n = rows[0].shape[1]
    at = iota((total, n), 0)
    out = jnp.zeros((total, n), F32)
    for k, row in enumerate(rows):
        out = jnp.where(at == k, jnp.broadcast_to(row.astype(F32), (total, n)), out)
    return out.astype(BF16)


def split_by(x, size):
    if size & (size - 1) == 0:
        return lax.shift_right_logical(x, jnp.int32(size.bit_length() - 1)), x & (size - 1)
    return x // size, x % size


def select(table, chosen):
    high, low = halves(table)
    both = dot(jnp.concatenate([high, low], axis=0), chosen)
    return both[: table.shape[0]] + both[table.shape[0] :]


def wide(one, two):
    blank = jnp.zeros(one.shape, BF16)

    def beside(first, second):
        upper = jnp.concatenate([first, blank], axis=1)
        return jnp.concatenate([upper, jnp.concatenate([blank, second], axis=1)], axis=0)

    (high, low), (high_two, low_two) = halves(one), halves(two)
    return beside(high, high_two), beside(low, low_two)


def pack_wide(chosen, parts):
    rows = chosen.shape[0] // 2
    pair = jnp.concatenate([chosen[:rows], chosen[rows:]], axis=1)
    return dot_nt(pair, parts[0]) + dot_nt(pair, parts[1])


def pack(chosen, x):
    return pack_wide(chosen, wide(x, x))


def unpack(packed):
    turned = packed.T
    middle = turned.shape[0] // 2
    return jnp.concatenate([turned[:middle], turned[middle:]], axis=1)


def kernel(
    n_clump, n_group, inner_clump, inner_group, cap, slots, half, stride,
    *refs,
):
    count_ref, *refs = refs
    sources, refs = refs[:INPUTS], refs[INPUTS:]
    got_ref, owned_of_ref, frac_out, other_ref, base_ref, patch_of_ref, answers_ref = refs[:7]
    tables, own, ask, asked, note, noted, fore, reply, back, send, recv = refs[7:18]
    send_sem, recv_sem, in_sem, known = refs[18:22]
    staged = refs[22:]
    (
        target_ref, lwt_ref, lgrid_ref, clu_ref, cwt_ref, pcol_ref, pwt_ref,
        scale_ref, pft_ref, flux_ref,
    ) = staged
    nv, patches = flux_ref.shape
    types = scale_ref.shape[0]
    cols = cwt_ref.shape[1]
    lus = lwt_ref.shape[1]
    cells = target_ref.shape[1]
    n = n_clump * n_group
    rows = n * stride
    outer_clump, outer_group = n_clump // inner_clump, n_group // inner_group
    places, askers = inner_clump * outer_group, outer_clump * inner_group
    sharers = places * inner_group
    pairs = sharers // 2
    field_ref, frac_ref = own.at[pl.ds(0, nv)], own.at[pl.ds(nv, 1)]
    loads = [
        pltpu.make_async_copy(source, into, in_sem.at[0 if k == 0 else 2 if k < 10 else 1])
        for k, (source, into) in enumerate(zip(sources, (*staged, frac_ref, field_ref)))
    ]
    my_clump, my_group = lax.axis_index("clump"), lax.axis_index("grp")
    my_slab, my_row = lax.div(my_clump, inner_clump), lax.rem(my_clump, inner_clump)
    my_side, my_core = lax.div(my_group, inner_group), lax.rem(my_group, inner_group)
    keeper = inner_group - 1
    keeps = my_core == keeper

    def ahead_of(mine, step, size):
        there = mine + step
        return jnp.where(there >= size, there - size, there)

    def behind(mine, step, size):
        there = mine - step
        return jnp.where(there < 0, there + size, there)

    def offsets(act, outer, inner, own=False, far_first=False):
        if outer <= 8:
            steps = [(o, i) for o in range(outer) for i in range(inner) if own or o or i]
            for o, i in steps[::-1] if far_first else steps:
                act(o * inner + i, o, i)
        else:
            for i in range(0 if own else 1, inner):
                act(i, 0, i)

            @pl.loop(1, outer)
            def _(o):
                for i in range(inner):
                    act(o * inner + i, o, i)

    def place(there, row, side, slab, core):
        slab, row = there(my_slab, slab, outer_clump), there(my_row, row, inner_clump)
        side, core = there(my_side, side, outer_group), there(my_core, core, inner_group)
        return slab * inner_clump + row, side * inner_group + core

    def each_other(act, there):
        for row in range(inner_clump - 1, -1, -1):
            for side in range(outer_group - 1, -1, -1):
                t = row * outer_group + side

                def one(block, o, i, t=t, row=row, side=side):
                    act(t * askers + block, place(there, row, side, o, i))

                offsets(one, outer_clump, inner_group, own=t > 0)

    def remote(source, into, k, device):
        sent = 1 if k == 3 else 0
        pltpu.make_async_remote_copy(
            src_ref=source,
            dst_ref=into,
            send_sem=send_sem.at[sent],
            recv_sem=recv_sem.at[k],
            device_id=device,
            device_id_type=MESH,
        ).start()

    def wait(rest, sem):
        pltpu.make_async_copy(rest, rest, sem).wait()

    barrier = pltpu.get_barrier_semaphore()

    def signal(sem, device):
        pl.semaphore_signal(sem, inc=1, device_id=device, device_id_type=MESH)

    def each_place(act, there):
        def one(block, o, i):
            act(block, place(there, o, i, 0, 0))

        offsets(one, inner_clump, outer_group, far_first=True)

    def against(block):
        o, i = block // outer_group, block % outer_group
        row, side = ahead_of(my_row, o, inner_clump), ahead_of(my_side, i, outer_group)
        return (row >= my_row) & (side >= my_side), (row <= my_row) & (side <= my_side)

    def slabs(act):
        if outer_clump <= 8:
            for o in range(1, outer_clump):
                act(o)
        else:
            pl.loop(1, outer_clump)(act)

    def each_slab(act, there):
        slabs(lambda o: act(o, place(there, 0, 0, o, 0)))

    def core_of(device, core):
        return device[0], device[1] - my_core + core

    def keeper_of(device):
        return core_of(device, keeper)

    here = (my_clump, my_group)
    last_place = (my_row == inner_clump - 1) & (my_side == outer_group - 1)
    last_plane = my_slab == outer_clump - 1
    last_chip = last_place & last_plane
    last = last_chip & keeps

    def greet(block, device):
        signal(barrier, keeper_of(device))

        @pl.when(against(block)[0])
        def _():
            for core in range(keeper):
                signal(barrier, core_of(device, core))

    @pl.when(keeps)
    def _():
        each_slab(lambda o, device: signal(barrier, keeper_of(device)), ahead_of)
        each_place(greet, ahead_of)
        for core in range(keeper):
            signal(barrier, core_of(here, core))

    @pl.when(jnp.logical_not(keeps))
    def _():
        signal(barrier, keeper_of(here))

    @pl.when(jnp.logical_not(keeps & (last_place | last_plane) | last_chip))
    def _():
        signal(barrier, (n_clump - 1, n_group - 1))

    for k in (0, 10, 11, *range(1, 10)):
        loads[k].start()

    table_rows = pl.ds(0, nv + 1)

    def share(block, device, direct=False):
        at = block * inner_group + my_core
        if direct:
            remote(sources[11], tables.at[at, pl.ds(0, nv)], 0, keeper_of(device))
            remote(sources[10], tables.at[at, pl.ds(nv, 1)], 0, keeper_of(device))
        else:
            remote(own.at[table_rows], tables.at[at, table_rows], 0, keeper_of(device))

    def get_own():
        loads[10].wait()
        loads[11].wait()

    def enter_keeper():
        get_own()
        near = places - 1 + outer_clump - 1 + keeper
        pl.semaphore_wait(barrier, jnp.where(last, n - 1, near))
        each_place(share, ahead_of)
        for core in range(keeper):
            signal(known.at[0], core_of(here, core))

        @pl.when(last)
        def _():
            each_other(lambda block, device: signal(known.at[1], device), ahead_of)

    def enter_other(direct):
        pl.semaphore_wait(barrier, (my_row + 1) * (my_side + 1))

        def share_lower(block, device):
            pl.when(against(block)[1])(lambda: share(block, device, direct))

        each_place(share_lower, ahead_of)
        share(0, here, direct)

    pl.when(last)(enter_keeper)
    pl.when(last_chip & jnp.logical_not(keeps))(lambda: enter_other(True))
    loads[0].wait()
    target = target_ref[...]
    owner, local = split_by(target, cells)
    owner_b = jnp.broadcast_to(owner.astype(F32), (cells, cells))
    same = owner_b == owner_b.T
    earlier = iota((cells, cells), 0) < iota((cells, cells), 1)
    rank = jnp.sum(jnp.where(same & earlier, 1.0, 0.0), axis=0, keepdims=True).astype(jnp.int32)
    to_clump, to_group = split_by(owner, n_group)
    to_slab, to_row = split_by(to_clump, inner_clump)
    to_side, to_core = split_by(to_group, inner_group)
    table = behind(my_row, to_row, inner_clump) * outer_group
    table = table + behind(my_side, to_side, outer_group)
    entry = table * inner_group + to_core
    slab = behind(to_slab, my_slab, outer_clump)
    wanted = (local + 1).astype(F32)
    asks = jnp.where(iota((outer_clump, cells), 0) == slab, wanted, 0.0).astype(BF16)
    ask_rows = dot_nt(asks, onehot(iota((128, cells), 0) == entry * slots + rank))
    for k in range(outer_clump):
        ask[k, 0:1, :] = ask_rows[k : k + 1]
    one_row = pl.ds(0, 1)
    pl.when(keeps & jnp.logical_not(last))(enter_keeper)
    pl.when(jnp.logical_not(keeps))(get_own)
    pl.when(jnp.logical_not(keeps | last_chip))(lambda: enter_other(False))

    def request(step, device):
        into = asked.at[step * inner_group + my_core, one_row]
        remote(ask.at[step, one_row], into, 1, keeper_of(device))

    @pl.when(jnp.logical_not(keeps))
    def _():
        request(0, here)

    @pl.when(jnp.logical_not(keeps))
    def _():
        pl.semaphore_wait(known.at[0], 1)

        def share_rest(block, device):
            pl.when(jnp.logical_not(against(block)[1]))(lambda: share(block, device))

        each_place(share_rest, ahead_of)

    each_slab(request, ahead_of)
    frac = frac_ref[...]
    block = behind(to_row, my_row, inner_clump) * outer_group
    block = (block + behind(to_side, my_side, outer_group)) * outer_clump + slab
    block = (block * inner_group + behind(to_core, my_core, inner_group)) * stride
    part, line = split_by(rank, half)
    slot_of = onehot(iota((2 * rows, cells), 0) == part * rows + block + line)
    asks = jnp.where(iota((rows, cells), 0) == block, wanted, 0.0).astype(BF16)
    id_rows = dot_nt(asks, onehot(iota((128, cells), 0) == rank))
    in_stride = split_by(iota((rows, 128), 0), stride)[1]
    note[...] = jnp.where(in_stride == 1, jnp.broadcast_to(frac, (rows, cells)), id_rows)
    noted[0:2, :] = note[0:2, :]

    def lines_of(block, count):
        start = block * stride
        return pl.ds(start if isinstance(start, int) else pl.multiple_of(start, stride), count)

    def give_note(block, device):
        its = lines_of(block, 2)
        remote(note.at[its], noted.at[its], 4, device)

    @pl.when(last_chip)
    def _():
        @pl.when(jnp.logical_not(last))
        def _():
            pl.semaphore_wait(known.at[1], 1)

        each_other(give_note, ahead_of)


    for load in loads[1:10]:
        load.wait()
    lu_hi, lu_lo = halves(lwt_ref[...])
    lu_rows = rows_of([lu_hi, lu_lo, lgrid_ref[...]], 16)
    lu_of = onehot(iota((lus, cols), 0) == clu_ref[...])
    col_vals = dot(lu_rows, lu_of)
    col_w = cwt_ref[...] * (col_vals[0:1] + col_vals[1:2])

    c_hi, c_lo = halves(col_w)
    col_rows = rows_of([c_hi, c_lo, col_vals[2:3]], 16)
    col_of = onehot(iota((cols, patches), 0) == pcol_ref[...])
    patch_vals = dot(col_rows, col_of)
    alive = jnp.where(iota((1, patches), 1) < count_ref[0], 1.0, 0.0)
    weight = alive * pwt_ref[...] * (patch_vals[0:1] + patch_vals[1:2])
    home = patch_vals[2:3].astype(jnp.int32)
    home_of = onehot(iota((cells, patches), 0) == home)

    scales = scale_ref[...]
    t1 = scales.astype(BF16).astype(F32)
    t2 = (scales - t1).astype(BF16).astype(F32)
    t3 = scales - t1 - t2
    pad = 128 - 3 * types
    stacked = jnp.concatenate([t1, t2, t3, jnp.zeros((pad, nv), F32)], axis=0)
    stacked = jnp.concatenate([stacked, jnp.zeros((128, 128 - nv), F32)], axis=1)
    scale_t = stacked.T[:nv].astype(BF16)
    kind = iota((128, patches), 0)
    type_of = onehot(
        (kind == pft_ref[...])
        | (kind == pft_ref[...] + types)
        | (kind == pft_ref[...] + 2 * types)
    )
    scaled = flux_ref[...] * dot(scale_t, type_of)

    x_hi, x_lo = halves(scaled * weight)
    w_hi, w_lo = halves(weight)
    sums = dot_nt(
        jnp.concatenate([x_hi, x_lo, rows_of([w_hi, w_lo], 16)], axis=0), home_of
    )
    num = sums[:nv] + sums[nv : 2 * nv]
    den = sums[2 * nv : 2 * nv + 1] + sums[2 * nv + 1 : 2 * nv + 2]
    mean = num / jnp.maximum(den, 1.0)

    send[...] = pack(slot_of, mean)
    recv[0:half, :] = send[0:half, :]
    @pl.when(jnp.logical_not(last_chip))
    def _():
        pl.semaphore_wait(known.at[1], 1)
        each_other(give_note, ahead_of)

    def give(block, device):
        its = lines_of(block, half)
        remote(send.at[its], recv.at[its], 2, device)

    each_other(give, ahead_of)

    @pl.when(keeps)
    def _():
        asked[keeper, 0:1, :] = ask[0, 0:1, :]
        wait(asked.at[pl.ds(0, askers - 1), one_row], recv_sem.at[1])

        def picks(told, count):
            height = count * slots
            told = jnp.broadcast_to(told, (count, slots, 128)).reshape(height, 128)
            lane_less = iota((height, 128), 1) - split_by(iota((height, 128), 0), slots)[1]
            spread = [jnp.where(lane_less == t * slots, told, 0.0) for t in range(sharers)]
            ids = dot(jnp.concatenate(spread, axis=0).astype(BF16), jnp.ones((128, cells), BF16))
            return onehot(ids == (iota(ids.shape, 1) + 1).astype(F32))

        def fill(into, chosen, count):
            for p in range(pairs):
                one, end = 2 * p * count * slots, 2 * (p + 1) * count * slots
                packed = pack_wide(chosen[one:end], held[p])
                into[:, p * slots : (p + 1) * slots, :] = packed.reshape(count, slots, 128)

        first = pl.ds(my_slab * inner_group, inner_group)
        first_picks = picks(asked[first, 0:1, :], inner_group)
        wait(tables.at[pl.ds(0, sharers - 1), table_rows], recv_sem.at[0])
        held = [own if t == keeper else tables.at[t] for t in range(sharers)]
        held = [(1.0 - x[nv : nv + 1, :]) * x[0:nv, :] for x in held]
        held = [wide(held[2 * p], held[2 * p + 1]) for p in range(pairs)]
        fill(fore, first_picks, inner_group)
        for i in range(inner_group):

            @pl.when((my_slab > 0) | (i < keeper))
            def _(i=i):
                remote(fore.at[i], back.at[my_slab], 3, (my_row, my_group - my_core + i))

        fill(reply, picks(asked[:, 0:1, :], askers), askers)

        def respond(o):
            clump, group = place(behind, 0, 0, o, 0)
            for i in range(keeper if isinstance(o, int) and o == 0 else inner_group):
                source = reply.at[o * inner_group + i]
                remote(source, back.at[o], 3, (clump, group - my_core + i))

        def respond_rest(o):
            pl.when(my_slab != o)(lambda: respond(o))

        respond_rest(0)
        slabs(respond_rest)
        back[0] = reply[keeper]

    other_ref[...] = (1.0 - frac) * field_ref[...]
    frac_out[...] = frac
    pair, side = split_by(entry, 2)
    answers = outer_clump * pairs * slots
    spot = side * answers + (slab * pairs + pair) * slots + rank
    answer_of = onehot(iota((2 * answers, cells), 0) == spot)
    patch_of_ref[...] = (dot(answer_of, home_of) * alive).astype(BF16)

    flat = pl.ds(0, (n - 1) * half)
    keeps_or_not = ((keeps, 1), (jnp.logical_not(keeps), 0))
    for which, first in keeps_or_not:

        @pl.when(which)
        def _(first=first):
            wait(tables.at[pl.ds(0, places - first), table_rows], send_sem.at[0])
            wait(ask.at[pl.ds(0, outer_clump - first), one_row], send_sem.at[0])

    wait(send.at[flat], send_sem.at[0])
    wait(note.at[pl.ds(0, (n - 1) * 2)], send_sem.at[0])
    wait(noted.at[pl.ds(0, (n - 1) * 2)], recv_sem.at[4])
    lane = iota((2 * rows, 128), 0)
    lane_part = jnp.where(lane >= rows, 1, 0)
    lane_line = split_by(lane - lane_part * rows, stride)[1]
    its_lane = (lane_line < half) & (
        iota((2 * rows, 128), 1) == lane_part * half + lane_line
    )
    told = jnp.where(in_stride < 2, noted[...], 0.0)
    ids_of = jnp.broadcast_to(told.reshape(n, stride, 128)[:, 0:1, :], (n, stride, 128)).reshape(rows, 128)
    spread = jnp.where(its_lane, jnp.concatenate([ids_of, ids_of], axis=0), 0.0).astype(BF16)
    ids = dot(spread, jnp.ones((128, cells), BF16))
    owned_of_ref[...] = onehot(ids == (iota((2 * rows, cells), 1) + 1).astype(F32))

    back_of = (table * outer_clump + behind(my_slab, to_slab, outer_clump)) * inner_group
    back_of = (back_of + behind(my_core, to_core, inner_group)) * stride + 1
    all_frac = select(told.T, onehot(iota((rows, cells), 0) == back_of))
    cell_frac = jnp.sum(
        jnp.where(iota((128, cells), 0) == local, all_frac, 0.0), axis=0, keepdims=True
    )
    base_ref[...] = alive * (scaled - select(cell_frac * mean, home_of))

    @pl.when(keeps)
    def _():
        wait(reply.at[pl.ds(0, askers - 1)], send_sem.at[1])

    for which, first in keeps_or_not:

        @pl.when(which)
        def _(first=first):
            wait(back.at[pl.ds(first, outer_clump - first)], recv_sem.at[3])

    wait(recv.at[flat], recv_sem.at[2])
    in_half = split_by(iota((rows, 128), 0), stride)[1] < half
    got_ref[...] = jnp.where(in_half, recv[...], 0.0)
    answers_ref[...] = back[...].reshape(answers, 128)


def store_kernel(
    got, owned_of, frac, other, base, patch_of, answers,
    merged_out, anomaly_out, merged, anomaly, sem,
):
    chunks = anomaly.shape[0]
    width = anomaly.shape[2]
    stores = []
    high, low = halves(unpack(answers[...]))
    table = jnp.concatenate([high, low], axis=0)
    for k in range(chunks):
        its = pl.ds(k * width, width)
        both = dot(table, patch_of[:, its])
        anomaly[k] = base[:, its] - (both[: high.shape[0]] + both[high.shape[0] :])
        stores.append(pltpu.make_async_copy(anomaly.at[k], anomaly_out.at[:, its], sem.at[k]))
        stores[-1].start()
    merged[...] = frac[...] * select(unpack(got[...]), owned_of[...]) + other[...]
    stores.append(pltpu.make_async_copy(merged, merged_out, sem.at[chunks]))
    stores[-1].start()
    for store in stores:
        store.wait()


def per_device(
    flux, patch_pft, patch_wt, patch_col, col_wt, col_lu, lu_wt, lu_grid, cell_target,
    patch_count, pft_scale, cpl_frac, cpl_field,
):
    n_clump = lax.axis_size("clump")
    n_group = lax.axis_size("grp")
    n = n_clump * n_group
    nv = flux.shape[2]
    patches = flux.shape[1]
    cells = cell_target.shape[1]
    inner_group = 2 if n_group % 2 == 0 else 1
    outer_group = n_group // inner_group
    inner_clump = outer_group if n_clump % outer_group == 0 else 1
    sharers = inner_clump * n_group
    outer_clump = n_clump // inner_clump
    askers = outer_clump * inner_group
    cap = max(2, 2 * cells // n)
    half = -(-cap // 2)
    slots = -(-cap // 8) * 8
    stride = -(-half // 8) * 8
    answers = outer_clump * (sharers // 2) * slots
    chunks = 2
    vmem = pl.BlockSpec(memory_space=pltpu.VMEM)
    hbm = pl.BlockSpec(memory_space=pltpu.HBM)
    staged = (
        cell_target, lu_wt, lu_grid, col_lu, col_wt, patch_col, patch_wt,
        pft_scale, patch_pft, flux[0].T,
    )
    inputs = (*staged, cpl_frac.reshape(1, -1), cpl_field.T)
    shapes = (
        jax.ShapeDtypeStruct((nv, cells), F32),
        jax.ShapeDtypeStruct((nv, patches), F32),
    )
    results = pl.pallas_call(
        functools.partial(
            kernel, n_clump, n_group, inner_clump, inner_group, cap, slots, half, stride
        ),
        out_shape=(
            pltpu.VMEM((n * stride, 128), F32),
            pltpu.VMEM((2 * n * stride, cells), BF16),
            pltpu.VMEM((1, cells), F32),
            pltpu.VMEM((nv, cells), F32),
            pltpu.VMEM((nv, patches), F32),
            pltpu.VMEM((2 * answers, patches), BF16),
            pltpu.VMEM((answers, 128), F32),
        ),
        in_specs=[pl.BlockSpec(memory_space=pltpu.SMEM)] + [hbm] * INPUTS,
        out_specs=(vmem,) * 7,
        scratch_shapes=[
            pltpu.VMEM((sharers, -(-(nv + 1) // 8) * 8, cells), F32),
            pltpu.VMEM((-(-(nv + 1) // 8) * 8, cells), F32),
            pltpu.VMEM((outer_clump, 8, 128), F32),
            pltpu.VMEM((askers, 8, 128), F32),
            pltpu.VMEM((n * stride, 128), F32),
            pltpu.VMEM((n * stride, 128), F32),
            pltpu.VMEM((inner_group, sharers // 2 * slots, 128), F32),
            pltpu.VMEM((askers, sharers // 2 * slots, 128), F32),
            pltpu.VMEM((outer_clump, sharers // 2 * slots, 128), F32),
            pltpu.VMEM((n * stride, 128), F32),
            pltpu.VMEM((n * stride, 128), F32),
            pltpu.SemaphoreType.DMA((2,)),
            pltpu.SemaphoreType.DMA((5,)),
            pltpu.SemaphoreType.DMA((3,)),
            pltpu.SemaphoreType.REGULAR((2,)),
        ]
        + [pltpu.VMEM(x.shape, x.dtype) for x in staged],
        compiler_params=pltpu.CompilerParams(
            collective_id=0, has_side_effects=True, vmem_limit_bytes=48 * 1024 * 1024
        ),
    )(patch_count, *[pltpu.with_memory_space_constraint(x, pltpu.HBM) for x in inputs])
    merged, anomaly = pl.pallas_call(
        store_kernel,
        out_shape=shapes,
        in_specs=[vmem] * 7,
        out_specs=(hbm, hbm),
        scratch_shapes=[
            pltpu.VMEM((nv, cells), F32),
            pltpu.VMEM((chunks, nv, patches // chunks), F32),
            pltpu.SemaphoreType.DMA((chunks + 1,)),
        ],
        compiler_params=pltpu.CompilerParams(vmem_limit_bytes=8 * 1024 * 1024),
    )(*results)
    return merged.T, anomaly.T[None]


def solution(mesh):
    split = P(("clump", "grp"))
    return jax.shard_map(
        per_device,
        mesh=mesh,
        in_specs=(split,) * 10 + (P(),) + (split,) * 2,
        out_specs=(split, split),
        check_vma=False,
    )
```
